32 devices in a mesh: dp: 8 (over y, x, core), ctx: 4 (over z).
Axes of the slice: x: 2, y: 2, z: 4, core: 2. Of those that a mesh axis runs over, the one named last changes fastest.
Arguments:
- tokens: bfloat16 [8, 32, 16, 3072], P('dp', 'ctx'), may hold values from -6 to 6
- modulation: float32 [8, 3, 3072], P('dp'), may hold values from -3 to 3
- query_key_value_weight: bfloat16 [3072, 1536], P('dp'), may hold values from -0.109375 to 0.109375
- output_projection_weight: bfloat16 [512, 3072], P(None, 'dp'), may hold values from -0.25 to 0.25
- adapter_down_maps: bfloat16 [3072, 64], P('dp'), may hold values from -0.109375 to 0.109375
- adapter_up_maps: bfloat16 [64, 512], P('dp'), may hold values from -1 to 1
- output_gradient: bfloat16 [8, 32, 16, 3072], P('dp', 'ctx'), may hold values from -6 to 6
Outputs:
- mixed_out: bfloat16 [8, 32, 16, 3072], P('dp', 'ctx')
- tokens_grad: bfloat16 [8, 32, 16, 3072], P('dp', 'ctx')
- modulation_grad: float32 [8, 3, 3072], P('dp')
- down_grad: float32 [3072, 64], P('dp')
- up_grad: float32 [64, 512], P('dp')
The draws below stay inside these ranges and needn't reach their ends.
All inputs are finite; a program needn't handle non-finite values.
Results may differ from the reference program's by a relative error of at most 0.019.
Values may be sent and summed in bfloat16 or wider, within the bound.
A program may use at most 128 MiB of HBM per device.

```python
import jax
import jax.numpy as jnp
from jax import lax

MODEL_WIDTH = 3072
LOCAL_HEADS = 4
HEAD_SIZE = 128
ADAPTER_RANK = 32
FRAMES = 32
CLIPS = 8
POS = 16
TOKENS = 4096


def steps_of(own_key, dims, cuts, low, high):
    loudness = 1.0
    for position, blocks in cuts:
        heights = jax.random.uniform(jax.random.fold_in(jax.random.fold_in(own_key, 6), position), (blocks,), jnp.float32, low / len(cuts), high / len(cuts))
        loudness = loudness * jnp.repeat(jnp.exp(heights), dims[position] // blocks).reshape((-1,) + (1,) * (len(dims) - 1 - position))
    return loudness


def normal_values(rng, dims, width, bound, pieces=(), held_as=jnp.bfloat16):
    factor_of = steps_of(rng, dims, pieces, -0.22, 0.18) if pieces else 1.0
    array = jax.random.normal(rng, dims, jnp.float32) * width * factor_of
    return jnp.minimum(jnp.maximum(array, -bound), bound).astype(held_as)


def setup_inputs(seed: int = 0) -> dict:
    seeds = jax.random.split(jax.random.key(seed), 8)
    tokens = normal_values(seeds[0], (CLIPS, FRAMES, POS, MODEL_WIDTH), 1.0, 6.0, ((0, 8), (1, 4)))
    modulation = normal_values(seeds[1], (CLIPS, 3, MODEL_WIDTH), 0.5, 3.0, ((0, 8),), jnp.float32)
    query_key_value_weight = normal_values(seeds[2], (MODEL_WIDTH, 3 * LOCAL_HEADS * HEAD_SIZE), MODEL_WIDTH ** -0.5, 0.109375, ((0, 8),))
    output_projection_weight = normal_values(seeds[3], (LOCAL_HEADS * HEAD_SIZE, MODEL_WIDTH), (LOCAL_HEADS * HEAD_SIZE) ** -0.5, 0.25, ((1, 8),))
    adapter_down_maps = normal_values(seeds[4], (MODEL_WIDTH, 2 * ADAPTER_RANK), MODEL_WIDTH ** -0.5, 0.109375, ((0, 8),))
    adapter_up_maps = normal_values(seeds[5], (2 * ADAPTER_RANK, LOCAL_HEADS * HEAD_SIZE), ADAPTER_RANK ** -0.5, 1.0, ((0, 8),))
    output_gradient = normal_values(seeds[6], (CLIPS, FRAMES, POS, MODEL_WIDTH), 1.0, 6.0, ((0, 8), (1, 4)))
    return {"tokens": tokens, "modulation": modulation, "query_key_value_weight": query_key_value_weight, "output_projection_weight": output_projection_weight, "adapter_down_maps": adapter_down_maps, "adapter_up_maps": adapter_up_maps, "output_gradient": output_gradient}


EPSILON = 1e-06

def times_transposed(left, right):
    return lax.dot_general(left, right, (((1,), (1,)), ((), ())), preferred_element_type=jnp.float32)

def transposed_times(left, right):
    return lax.dot_general(left, right, (((0,), (0,)), ((), ())), preferred_element_type=jnp.float32)

def normalize_rows(flat_tokens, modulation_per_clip):
    values = flat_tokens.astype(jnp.float32)
    center = values - lax.optimization_barrier(jnp.mean(values, -1, keepdims=True))
    inverse_value = lax.rsqrt(lax.optimization_barrier(jnp.mean(center * center, -1, keepdims=True)) + EPSILON)
    normalized_input = center * inverse_value
    hidden_state = (normalized_input * (1.0 + modulation_per_clip[1]) + modulation_per_clip[0]).astype(jnp.bfloat16)
    return (normalized_input, inverse_value, hidden_state)

def projection_forward(hidden_state, qkv_full, down_full, up_full, adapter_inner_rank):
    head_size_value = up_full.shape[1]
    base_proj = jnp.dot(hidden_state, qkv_full, preferred_element_type=jnp.float32)
    low_rank_product = jnp.dot(hidden_state, down_full, preferred_element_type=jnp.float32).astype(jnp.bfloat16)
    delta_query = jnp.dot(low_rank_product[:, :adapter_inner_rank], up_full[:adapter_inner_rank], preferred_element_type=jnp.float32)
    delta_value = jnp.dot(low_rank_product[:, adapter_inner_rank:], up_full[adapter_inner_rank:], preferred_element_type=jnp.float32)
    query_unnormalized = base_proj[:, :head_size_value] + delta_query
    key_unnormalized = base_proj[:, head_size_value:2 * head_size_value]
    value_row_matrix = (base_proj[:, 2 * head_size_value:] + delta_value).astype(jnp.bfloat16)
    return (low_rank_product, query_unnormalized, key_unnormalized, value_row_matrix)

def head_stats(raw_rows, head_dim):
    grouped = raw_rows.reshape(raw_rows.shape[0], -1, head_dim)
    inverse_value = lax.rsqrt(lax.optimization_barrier(jnp.mean(grouped * grouped, -1, keepdims=True)) + EPSILON)
    return (grouped, inverse_value)

def head_normed(raw_rows, head_dim):
    grouped, inverse_value = head_stats(raw_rows, head_dim)
    return (grouped * inverse_value).reshape(raw_rows.shape).astype(jnp.bfloat16)

def head_norm_back(raw_rows, incoming_grad, head_dim):
    grouped, inverse_value = head_stats(raw_rows, head_dim)
    incoming = incoming_grad.astype(jnp.float32).reshape(grouped.shape)
    inner_mean = lax.optimization_barrier(jnp.mean(grouped * incoming, -1, keepdims=True))
    return (inverse_value * incoming - grouped * inverse_value ** 3 * inner_mean).reshape(raw_rows.shape)

def split_heads(rows_in, head_dim):
    frame_count, place_count, head_size_value = rows_in.shape
    return rows_in.reshape(frame_count, place_count, head_size_value // head_dim, head_dim).astype(jnp.float32)

def attend(query_rows, key_rows, value_row_matrix, head_dim):
    score_scale = head_dim ** (-0.5)
    query_heads = split_heads(query_rows, head_dim)
    key_heads = split_heads(key_rows, head_dim)
    value_heads = split_heads(value_row_matrix, head_dim)
    scores = jnp.einsum('fphd,gphd->phfg', query_heads, key_heads) * score_scale
    expo = jnp.exp(scores)
    attention_weights = expo / lax.optimization_barrier(jnp.sum(expo, -1, keepdims=True))
    weights_low = attention_weights.astype(jnp.bfloat16).astype(jnp.float32)
    attended = jnp.einsum('phfg,gphd->fphd', weights_low, value_heads).astype(jnp.bfloat16)
    return (attended.reshape(query_rows.shape), attention_weights)

def attend_back(attended_grad, attention_weights, query_rows, key_rows, value_row_matrix, head_dim):
    score_scale = head_dim ** (-0.5)
    grad_heads = split_heads(attended_grad, head_dim)
    query_heads = split_heads(query_rows, head_dim)
    key_heads = split_heads(key_rows, head_dim)
    value_heads = split_heads(value_row_matrix, head_dim)
    weights_low = attention_weights.astype(jnp.bfloat16).astype(jnp.float32)
    prob_grad = jnp.einsum('fphd,gphd->phfg', grad_heads, value_heads)
    value_gradient = jnp.einsum('phfg,fphd->gphd', weights_low, grad_heads).astype(jnp.bfloat16)
    score_grad = attention_weights * (prob_grad - lax.optimization_barrier(jnp.sum(attention_weights * prob_grad, -1, keepdims=True)))
    score_low = (score_grad * score_scale).astype(jnp.bfloat16).astype(jnp.float32)
    query_grad = jnp.einsum('phfg,gphd->fphd', score_low, key_heads).astype(jnp.bfloat16)
    key_grad = jnp.einsum('phfg,fphd->gphd', score_low, query_heads).astype(jnp.bfloat16)
    shape_rows = query_rows.shape
    return (query_grad.reshape(shape_rows), key_grad.reshape(shape_rows), value_gradient.reshape(shape_rows))

def projection_backward(query_normalized_gradient, key_normalized_gradient, value_gradient, query_unnormalized, key_unnormalized, hidden_state, low_rank_product, normalized_input, inverse_value, modulation_per_clip, qkv_full, down_full, up_full, adapter_inner_rank, head_dim):
    head_size_value = up_full.shape[1]
    query_back = head_norm_back(query_unnormalized, query_normalized_gradient, head_dim)
    key_back = head_norm_back(key_unnormalized, key_normalized_gradient, head_dim)
    joined_grad = jnp.concatenate([query_back, key_back, value_gradient.astype(jnp.float32)], 1).astype(jnp.bfloat16)
    query_block = joined_grad[:, :head_size_value]
    value_block = joined_grad[:, 2 * head_size_value:]
    up_grad = jnp.concatenate([transposed_times(low_rank_product[:, :adapter_inner_rank], query_block), transposed_times(low_rank_product[:, adapter_inner_rank:], value_block)], 0)
    low_grad = jnp.concatenate([times_transposed(query_block, up_full[:adapter_inner_rank]), times_transposed(value_block, up_full[adapter_inner_rank:])], 1).astype(jnp.bfloat16)
    hidden_grad = times_transposed(joined_grad, qkv_full) + times_transposed(low_grad, down_full)
    down_grad = transposed_times(hidden_state, low_grad)
    shift_gradient = lax.optimization_barrier(jnp.sum(hidden_grad, 0))
    scale_gradient = lax.optimization_barrier(jnp.sum(hidden_grad * normalized_input, 0))
    normed_grad = hidden_grad * (1.0 + modulation_per_clip[1])
    first_mean = lax.optimization_barrier(jnp.mean(normed_grad, -1, keepdims=True))
    second_mean = lax.optimization_barrier(jnp.mean(normed_grad * normalized_input, -1, keepdims=True))
    token_gradient_rows = inverse_value * (normed_grad - first_mean - normalized_input * second_mean)
    return (token_gradient_rows, shift_gradient, scale_gradient, down_grad, up_grad)

def reference(tokens, modulation, query_key_value_weight, output_projection_weight, adapter_down_maps, adapter_up_maps, output_gradient):
    head_size_value = LOCAL_HEADS * HEAD_SIZE
    frame_shape = (FRAMES, POS, head_size_value)

    def clip_pass(inputs):
        tokens_clip, modulation_per_clip, upstream_clip = inputs
        flat_tokens = tokens_clip.reshape(-1, MODEL_WIDTH)
        normalized_input, inverse_value, hidden_state = normalize_rows(flat_tokens, modulation_per_clip)
        low_rank_product, query_unnormalized, key_unnormalized, value_row_matrix = projection_forward(hidden_state, query_key_value_weight, adapter_down_maps, adapter_up_maps, ADAPTER_RANK)
        query_rows = head_normed(query_unnormalized, HEAD_SIZE)
        key_rows = head_normed(key_unnormalized, HEAD_SIZE)
        attended, attention_weights = attend(query_rows.reshape(frame_shape), key_rows.reshape(frame_shape), value_row_matrix.reshape(frame_shape), HEAD_SIZE)
        branch_out = jnp.dot(attended.reshape(-1, head_size_value), output_projection_weight, preferred_element_type=jnp.float32)
        mixed_out = (flat_tokens.astype(jnp.float32) + modulation_per_clip[2] * branch_out).astype(jnp.bfloat16)
        upstream = upstream_clip.reshape(-1, MODEL_WIDTH).astype(jnp.float32)
        gate_grad = lax.optimization_barrier(jnp.sum(upstream * branch_out, 0))
        branch_grad = (upstream * modulation_per_clip[2]).astype(jnp.bfloat16)
        attended_grad = times_transposed(branch_grad, output_projection_weight).astype(jnp.bfloat16)
        query_normalized_gradient, key_normalized_gradient, value_gradient = attend_back(attended_grad.reshape(frame_shape), attention_weights, query_rows.reshape(frame_shape), key_rows.reshape(frame_shape), value_row_matrix.reshape(frame_shape), HEAD_SIZE)
        token_gradient_rows, shift_gradient, scale_gradient, down_section, up_section = projection_backward(query_normalized_gradient.reshape(-1, head_size_value), key_normalized_gradient.reshape(-1, head_size_value), value_gradient.reshape(-1, head_size_value), query_unnormalized, key_unnormalized, hidden_state, low_rank_product, normalized_input, inverse_value, modulation_per_clip, query_key_value_weight, adapter_down_maps, adapter_up_maps, ADAPTER_RANK, HEAD_SIZE)
        tokens_grad = (upstream + token_gradient_rows).astype(jnp.bfloat16)
        modulation_part = jnp.stack([shift_gradient, scale_gradient, gate_grad], 0)
        return (mixed_out.reshape(tokens_clip.shape), tokens_grad.reshape(tokens_clip.shape), modulation_part, down_section, up_section)
    mixed_out, tokens_grad, modulation_parts, down_parts, up_parts = lax.map(clip_pass, (tokens, modulation, output_gradient))
    grad_scale = TOKENS ** (-0.5)
    return (mixed_out, tokens_grad, modulation_parts * grad_scale, lax.optimization_barrier(jnp.sum(down_parts, 0)) * grad_scale, lax.optimization_barrier(jnp.sum(up_parts, 0)) * grad_scale)
```

```python
import functools

import jax
import jax.numpy as jnp
from jax import lax
from jax.experimental import pallas as pl
from jax.experimental.pallas import tpu as pltpu
from jax.sharding import PartitionSpec as P

HEAD_SIZE = 128


EPSILON = 1e-06


def times_transposed(left, right):
    return lax.dot_general(
        left, right, (((1,), (1,)), ((), ())), preferred_element_type=jnp.float32
    )


def transposed_times(left, right):
    return lax.dot_general(
        left, right, (((0,), (0,)), ((), ())), preferred_element_type=jnp.float32
    )


def normalize_rows(flat_tokens, modulation_per_clip):
    values = flat_tokens.astype(jnp.float32)
    center = values - jnp.mean(values, -1, keepdims=True)
    inverse_value = lax.rsqrt(jnp.mean(center * center, -1, keepdims=True) + EPSILON)
    normalized_input = center * inverse_value
    hidden_state = (
        normalized_input * (1.0 + modulation_per_clip[1]) + modulation_per_clip[0]
    ).astype(jnp.bfloat16)
    return (normalized_input, inverse_value, hidden_state)


def projection_forward(hidden_state, qkv_full, down_full, up_full, adapter_inner_rank):
    head_size_value = up_full.shape[1]
    base_proj = jnp.dot(hidden_state, qkv_full, preferred_element_type=jnp.float32)
    low_rank_product = jnp.dot(hidden_state, down_full, preferred_element_type=jnp.float32).astype(
        jnp.bfloat16
    )
    delta_query = jnp.dot(
        low_rank_product[:, :adapter_inner_rank],
        up_full[:adapter_inner_rank],
        preferred_element_type=jnp.float32,
    )
    delta_value = jnp.dot(
        low_rank_product[:, adapter_inner_rank:],
        up_full[adapter_inner_rank:],
        preferred_element_type=jnp.float32,
    )
    query_unnormalized = base_proj[:, :head_size_value] + delta_query
    key_unnormalized = base_proj[:, head_size_value : 2 * head_size_value]
    value_row_matrix = (base_proj[:, 2 * head_size_value :] + delta_value).astype(jnp.bfloat16)
    return (low_rank_product, query_unnormalized, key_unnormalized, value_row_matrix)


def head_stats(raw_rows, head_dim):
    grouped = raw_rows.reshape(raw_rows.shape[0], -1, head_dim)
    inverse_value = lax.rsqrt(jnp.mean(grouped * grouped, -1, keepdims=True) + EPSILON)
    return (grouped, inverse_value)


def head_normed(raw_rows, head_dim):
    grouped, inverse_value = head_stats(raw_rows, head_dim)
    return (grouped * inverse_value).reshape(raw_rows.shape).astype(jnp.bfloat16)


def head_norm_back(raw_rows, incoming_grad, head_dim):
    grouped, inverse_value = head_stats(raw_rows, head_dim)
    incoming = incoming_grad.astype(jnp.float32).reshape(grouped.shape)
    inner_mean = jnp.mean(grouped * incoming, -1, keepdims=True)
    return (inverse_value * incoming - grouped * inverse_value**3 * inner_mean).reshape(
        raw_rows.shape
    )


def split_heads(rows_in, head_dim):
    frame_count, place_count, head_size_value = rows_in.shape
    return rows_in.reshape(frame_count, place_count, head_size_value // head_dim, head_dim)


def attend(query_rows, key_rows, value_row_matrix, head_dim):
    score_scale = head_dim ** (-0.5)
    query_heads = split_heads(query_rows, head_dim)
    key_heads = split_heads(key_rows, head_dim)
    value_heads = split_heads(value_row_matrix, head_dim)
    scores = (
        jnp.einsum("fphd,gphd->phfg", query_heads, key_heads, preferred_element_type=jnp.float32)
        * score_scale
    )
    expo = jnp.exp(scores)
    attention_weights = expo / jnp.sum(expo, -1, keepdims=True)
    weights_low = attention_weights.astype(jnp.bfloat16)
    attended = jnp.einsum(
        "phfg,gphd->fphd", weights_low, value_heads, preferred_element_type=jnp.float32
    ).astype(jnp.bfloat16)
    return (attended.reshape(query_rows.shape), attention_weights)


def attend_back(attended_grad, attention_weights, query_rows, key_rows, value_row_matrix, head_dim):
    score_scale = head_dim ** (-0.5)
    grad_heads = split_heads(attended_grad, head_dim)
    query_heads = split_heads(query_rows, head_dim)
    key_heads = split_heads(key_rows, head_dim)
    value_heads = split_heads(value_row_matrix, head_dim)
    weights_low = attention_weights.astype(jnp.bfloat16)
    prob_grad = jnp.einsum(
        "fphd,gphd->phfg", grad_heads, value_heads, preferred_element_type=jnp.float32
    )
    value_gradient = jnp.einsum(
        "phfg,fphd->gphd", weights_low, grad_heads, preferred_element_type=jnp.float32
    ).astype(jnp.bfloat16)
    score_grad = attention_weights * (
        prob_grad - jnp.sum(attention_weights * prob_grad, -1, keepdims=True)
    )
    score_low = (score_grad * score_scale).astype(jnp.bfloat16)
    query_grad = jnp.einsum(
        "phfg,gphd->fphd", score_low, key_heads, preferred_element_type=jnp.float32
    ).astype(jnp.bfloat16)
    key_grad = jnp.einsum(
        "phfg,fphd->gphd", score_low, query_heads, preferred_element_type=jnp.float32
    ).astype(jnp.bfloat16)
    shape_rows = query_rows.shape
    return (
        query_grad.reshape(shape_rows),
        key_grad.reshape(shape_rows),
        value_gradient.reshape(shape_rows),
    )


def projection_backward(
    query_normalized_gradient,
    key_normalized_gradient,
    value_gradient,
    query_unnormalized,
    key_unnormalized,
    hidden_state,
    low_rank_product,
    normalized_input,
    inverse_value,
    modulation_per_clip,
    qkv_full,
    down_full,
    up_full,
    adapter_inner_rank,
    head_dim,
):
    head_size_value = up_full.shape[1]
    query_back = head_norm_back(query_unnormalized, query_normalized_gradient, head_dim)
    key_back = head_norm_back(key_unnormalized, key_normalized_gradient, head_dim)
    joined_grad = jnp.concatenate(
        [query_back, key_back, value_gradient.astype(jnp.float32)], 1
    ).astype(jnp.bfloat16)
    query_block = joined_grad[:, :head_size_value]
    value_block = joined_grad[:, 2 * head_size_value :]
    up_grad = jnp.concatenate(
        [
            transposed_times(low_rank_product[:, :adapter_inner_rank], query_block),
            transposed_times(low_rank_product[:, adapter_inner_rank:], value_block),
        ],
        0,
    )
    low_grad = jnp.concatenate(
        [
            times_transposed(query_block, up_full[:adapter_inner_rank]),
            times_transposed(value_block, up_full[adapter_inner_rank:]),
        ],
        1,
    ).astype(jnp.bfloat16)
    hidden_grad = times_transposed(joined_grad, qkv_full) + times_transposed(low_grad, down_full)
    down_grad = transposed_times(hidden_state, low_grad)
    shift_gradient = jnp.sum(hidden_grad, 0)
    scale_gradient = jnp.sum(hidden_grad * normalized_input, 0)
    normed_grad = hidden_grad * (1.0 + modulation_per_clip[1])
    first_mean = jnp.mean(normed_grad, -1, keepdims=True)
    second_mean = jnp.mean(normed_grad * normalized_input, -1, keepdims=True)
    token_gradient_rows = inverse_value * (
        normed_grad - first_mean - normalized_input * second_mean
    )
    return (token_gradient_rows, shift_gradient, scale_gradient, down_grad, up_grad)


def per_device(
    tokens,
    modulation,
    query_key_value_weight,
    output_projection_weight,
    adapter_down_maps,
    adapter_up_maps,
    output_gradient,
):
    adapter_inner_rank = adapter_down_maps.shape[1] // 2
    head_dim = HEAD_SIZE
    qkv_full, out_full, down_full, up_full = (
        lax.all_gather(query_key_value_weight, "dp", axis=0, tiled=True),
        lax.all_gather(output_projection_weight, "dp", axis=1, tiled=True),
        lax.all_gather(adapter_down_maps, "dp", axis=0, tiled=True),
        lax.all_gather(adapter_up_maps, "dp", axis=0, tiled=True),
    )
    head_size_value = up_full.shape[1]
    local_shape = tokens.shape
    frame_shape = (1, local_shape[1], local_shape[2], head_size_value)
    modulation_per_clip = modulation[0]
    flat_tokens = tokens.reshape(-1, local_shape[3])
    normalized_input, inverse_value, hidden_state = normalize_rows(flat_tokens, modulation_per_clip)
    low_rank_product, query_unnormalized, key_unnormalized, value_row_matrix = projection_forward(
        hidden_state, qkv_full, down_full, up_full, adapter_inner_rank
    )
    query_rows = head_normed(query_unnormalized, head_dim)
    key_rows = head_normed(key_unnormalized, head_dim)
    upstream = output_gradient.reshape(-1, local_shape[3]).astype(jnp.float32)
    branch_grad = (upstream * modulation_per_clip[2]).astype(jnp.bfloat16)
    attended_grad = (
        times_transposed(branch_grad, out_full).astype(jnp.bfloat16).reshape(frame_shape)
    )
    query_place, key_place, value_place = (
        lax.all_to_all(
            query_rows.reshape(frame_shape), "ctx", split_axis=2, concat_axis=1, tiled=True
        ),
        lax.all_to_all(
            key_rows.reshape(frame_shape), "ctx", split_axis=2, concat_axis=1, tiled=True
        ),
        lax.all_to_all(
            value_row_matrix.reshape(frame_shape), "ctx", split_axis=2, concat_axis=1, tiled=True
        ),
    )
    attended, attention_weights = attend(query_place[0], key_place[0], value_place[0], head_dim)
    attended_frames = lax.all_to_all(attended[None], "ctx", split_axis=1, concat_axis=2, tiled=True)
    grad_place = lax.all_to_all(attended_grad, "ctx", split_axis=2, concat_axis=1, tiled=True)
    query_normalized_gradient, key_normalized_gradient, value_gradient = attend_back(
        grad_place[0], attention_weights, query_place[0], key_place[0], value_place[0], head_dim
    )
    query_back_frames, key_back_frames, value_back_frames = (
        lax.all_to_all(
            query_normalized_gradient[None], "ctx", split_axis=1, concat_axis=2, tiled=True
        ),
        lax.all_to_all(
            key_normalized_gradient[None], "ctx", split_axis=1, concat_axis=2, tiled=True
        ),
        lax.all_to_all(value_gradient[None], "ctx", split_axis=1, concat_axis=2, tiled=True),
    )
    branch_out = jnp.dot(
        attended_frames.reshape(-1, head_size_value), out_full, preferred_element_type=jnp.float32
    )
    mixed_out = (flat_tokens.astype(jnp.float32) + modulation_per_clip[2] * branch_out).astype(
        jnp.bfloat16
    )
    gate_grad = jnp.sum(upstream * branch_out, 0)
    token_gradient_rows, shift_gradient, scale_gradient, down_section, up_section = (
        projection_backward(
            query_back_frames.reshape(-1, head_size_value),
            key_back_frames.reshape(-1, head_size_value),
            value_back_frames.reshape(-1, head_size_value),
            query_unnormalized,
            key_unnormalized,
            hidden_state,
            low_rank_product,
            normalized_input,
            inverse_value,
            modulation_per_clip,
            qkv_full,
            down_full,
            up_full,
            adapter_inner_rank,
            head_dim,
        )
    )
    tokens_grad = (upstream + token_gradient_rows).astype(jnp.bfloat16)
    token_total = lax.axis_size("dp") * lax.axis_size("ctx") * flat_tokens.shape[0]
    grad_scale = token_total ** (-0.5)
    modulation_part = jnp.stack([shift_gradient, scale_gradient, gate_grad], 0)[None] * grad_scale
    down_section = down_section * grad_scale
    up_section = up_section * grad_scale
    down_total, up_total, modulation_grad = (
        lax.psum(down_section.astype(jnp.bfloat16), "ctx").astype(jnp.float32),
        lax.psum(up_section.astype(jnp.bfloat16), "ctx").astype(jnp.float32),
        lax.psum(modulation_part.astype(jnp.bfloat16), "ctx").astype(jnp.float32),
    )
    down_grad, up_grad = (
        lax.psum_scatter(
            down_total.astype(jnp.bfloat16), "dp", scatter_dimension=0, tiled=True
        ).astype(jnp.float32),
        lax.psum_scatter(
            up_total.astype(jnp.bfloat16), "dp", scatter_dimension=0, tiled=True
        ).astype(jnp.float32),
    )
    return (
        mixed_out.reshape(local_shape),
        tokens_grad.reshape(local_shape),
        modulation_grad,
        down_grad,
        up_grad,
    )


BF16 = jnp.bfloat16
F32 = jnp.float32


def dot_nn(a, b):
    return lax.dot_general(a, b, (((1,), (0,)), ((), ())), preferred_element_type=F32)


def place(y, x, c):
    return y * 4 + x * 2 + c


def layer_kernel(
    dims,
    tokens_in, modulation_in, outgrad_in, qkv_in, out_in, down_in, up_in,
    mixed_out, tokens_grad, mod_out, down_out, up_out,
    tokens, modulation, outgrad, W, O, DT, U, H, N, BG, RAW, DS, DR, QS, QR, OS, OR, GS, GR,
    WT, LOW, JG, LG, HG, RS, RR, US, UR, ZD, ZU, ZM,
    load_sem, local_sem, gs_sem, gr_sem, ds_sem, dr_sem, qs_sem, qr_sem, os_sem, or_sem,
    bs_sem, br_sem, rs_sem, rr_sem, us_sem, ur_sem, zs_sem, zr_sem,
):
    ndp, nctx, rows, places, width, block, heads_width, rank2, total_tokens = dims
    nh = heads_width // HEAD_SIZE
    part = rows // nctx
    qkv_width = 3 * heads_width
    me = lax.axis_index("dp")
    mz = lax.axis_index("ctx")
    y, x, c = me // 4, (me // 2) % 2, me % 2
    y1, x1, c1 = 1 - y, 1 - x, 1 - c
    xn, yn, pt = place(y, x1, c), place(y1, x, c), place(y, x, c1)
    rel_owner = place((y + c) % 2, (x + 1 - c) % 2, c)
    rel_target = place((y + 1 - c) % 2, (x + c) % 2, c)
    oth_owner = rel_target
    diag = place(y1, x1, c)
    rel_r = 2 + 2 * c
    oth_r = 4 - 2 * c

    barrier = pltpu.get_barrier_semaphore()
    for t in range(1, ndp):
        pl.semaphore_signal(barrier, inc=1, device_id={"dp": lax.rem(me + t, ndp)}, device_id_type=pl.DeviceIdType.MESH)
    for t in range(1, nctx):
        pl.semaphore_signal(barrier, inc=1, device_id={"ctx": lax.rem(mz + t, nctx)}, device_id_type=pl.DeviceIdType.MESH)
    loads = []
    for t, (src, dst) in enumerate(((tokens_in, tokens), (outgrad_in, outgrad), (modulation_in, modulation))):
        load = pltpu.make_async_copy(src, dst, load_sem.at[t])
        load.start()
        loads.append(load)
    pl.semaphore_wait(barrier, ndp - 1 + nctx - 1)

    parity = mz % 2
    pair_z = mz + 1 - 2 * parity
    big = (block // 16) * 5 // 24 * 16
    rest = block - 4 * big
    items, near = 8, 6

    def view(ref, own, k):
        if k == 2:
            return out_in if own else O.at[ref]
        if k == 3:
            return down_in if own else DT.at[ref]
        if k == 4:
            return up_in if own else U.at[ref]
        if k == 5:
            span = pl.ds(0, rest)
        elif k < 2:
            span = pl.ds(pl.multiple_of(rest + (2 * parity + k) * big, 16), big)
        else:
            span = pl.ds(pl.multiple_of(rest + (2 * (1 - parity) + k - near) * big, 16), big)
        return qkv_in.at[span, :] if own else W.at[ref, span, :]

    def piece(owner, k):
        return view(owner, False, k)

    def own_piece(k):
        return view(me, True, k)

    def push(src, owner, k, target, s, r):
        return pltpu.make_async_remote_copy(
            src_ref=src, dst_ref=piece(owner, k), send_sem=gs_sem.at[s, k], recv_sem=gr_sem.at[r, k],
            device_id={"dp": target}, device_id_type=pl.DeviceIdType.MESH)

    def across(owner, k, s, r):
        return pltpu.make_async_remote_copy(
            src_ref=piece(owner, k), dst_ref=piece(owner, k), send_sem=gs_sem.at[s, k],
            recv_sem=gr_sem.at[r, near + k],
            device_id={"ctx": pair_z}, device_id_type=pl.DeviceIdType.MESH)

    def arrived(owner, k, r):
        push(piece(owner, k), owner, k, pt, 0, r).wait_recv()

    def forward(owner, k, s, r):
        push(piece(owner, k), owner, k, pt, s, r).start()

    def own_out(k):
        push(own_piece(k), me, k, xn, 0, 2).start()
        push(own_piece(k), me, k, yn, 1, 4).start()

    locals_ = []
    for k in (0, 1, 2):
        own_out(k)
    for k in range(items):
        copy = pltpu.make_async_copy(own_piece(k), piece(me, k), local_sem.at[k])
        copy.start()
        locals_.append(copy)
        push(own_piece(k), me, k, pt, 2, 1).start()

    def cols(j):
        return pl.ds(pl.multiple_of(j * block, 128), block)

    for load in loads:
        load.wait()

    def sum_body(j, s):
        return s + jnp.sum(tokens[:, cols(j)].astype(F32), -1, keepdims=True)

    mean = lax.fori_loop(0, ndp, sum_body, jnp.zeros((rows, 1), F32)) / width

    def var_body(j, s):
        d = tokens[:, cols(j)].astype(F32) - mean
        return s + jnp.sum(d * d, -1, keepdims=True)

    var = lax.fori_loop(0, ndp, var_body, jnp.zeros((rows, 1), F32)) / width
    rstd = lax.rsqrt(var + EPSILON)

    def norm_body(j, _):
        n = (tokens[:, cols(j)].astype(F32) - mean) * rstd
        N[j] = n
        H[j] = (n * (1.0 + modulation[1, :, cols(j)]) + modulation[0, :, cols(j)]).astype(BF16)
        BG[j] = (outgrad[:, cols(j)].astype(F32) * modulation[2, :, cols(j)]).astype(BF16)
        return 0

    lax.fori_loop(0, ndp, norm_body, 0)

    def from_sides(k):
        arrived(rel_owner, k, rel_r)
        push(piece(rel_owner, k), rel_owner, k, rel_target, 3, 6).start()
        if k < 2:
            across(rel_owner, k, 7, rel_r).start()
        forward(rel_owner, k, 4, 1 + rel_r)
        arrived(oth_owner, k, oth_r)
        if k < 2:
            across(oth_owner, k, 8, oth_r).start()
        forward(oth_owner, k, 5, 1 + oth_r)

    def from_diag(k):
        arrived(diag, k, 6)
        if k < 2:
            across(diag, k, 9, 6).start()
        forward(diag, k, 6, 7)

    pt_owners = ((pt, 1), (place(y, x1, c1), 3), (place(y1, x, c1), 5))
    last_owner = place(y1, x1, c1)

    def grad_part(owner):
        WT[...] += times_transposed(BG[owner], O[owner])

    def qkv_part(owner):
        RAW[...] += dot_nn(H[owner], W[owner])
        LOW[...] += times_transposed(H[owner], DT[owner])

    RAW[...] = jnp.zeros_like(RAW)
    LOW[...] = jnp.zeros_like(LOW)
    WT[...] = jnp.zeros_like(WT)
    for k in (0, 1):
        from_sides(k)
    for k in (3, 4, 5):
        own_out(k)
    for k in range(items):
        locals_[k].wait()
    grad_part(me)
    qkv_part(me)
    from_sides(2)
    for k in (0, 1):
        from_diag(k)
    for k in (3, 4, 5):
        from_sides(k)
    from_diag(2)
    for owner in (xn, yn):
        grad_part(owner)
    for owner, r in pt_owners:
        arrived(owner, 2, r)
        grad_part(owner)
    grad_part(diag)
    arrived(last_owner, 2, 7)
    grad_part(last_owner)

    def ctx_copy(src, dst, ssem, rsem, t):
        return pltpu.make_async_remote_copy(
            src_ref=src, dst_ref=dst, send_sem=ssem.at[t], recv_sem=rsem.at[t],
            device_id={"ctx": lax.rem(mz + t, nctx)}, device_id_type=pl.DeviceIdType.MESH)

    def exchange(sent, got, ssem, rsem):
        copies = []
        for t in range(1, nctx):
            copy = ctx_copy(sent.at[lax.rem(mz + t, nctx)], got.at[mz], ssem, rsem, t)
            copy.start()
            copies.append(copy)
        return copies

    frames = rows // places
    across_rows = lax.broadcasted_iota(jnp.int32, (rows, rows), 0)
    along_rows = lax.broadcasted_iota(jnp.int32, (rows, rows), 1)
    perm = jnp.where(
        along_rows == (across_rows % frames) * places + across_rows // frames, 1.0, 0.0
    ).astype(BF16)
    perm_back = jnp.where(
        across_rows == (along_rows % frames) * places + along_rows // frames, 1.0, 0.0
    ).astype(BF16)
    local_places = places // nctx
    same = jnp.where(
        (across_rows // frames) % local_places == (along_rows // frames) % local_places, 1.0, 0.0
    )

    def to_place(value):
        return dot_nn(perm, value).astype(BF16)

    def to_frame(value):
        return dot_nn(perm_back, value).astype(BF16)

    DS[...] = to_place(WT[...].astype(BF16)).reshape(nctx, part, heads_width)
    DR[mz] = DS[mz]
    grad_copies = exchange(DS, DR, ds_sem, dr_sem)

    for k in (near, near + 1):
        arrived(rel_owner, k, rel_r)
        forward(rel_owner, k, 4, 1 + rel_r)
        arrived(oth_owner, k, oth_r)
        forward(oth_owner, k, 5, 1 + oth_r)
    for owner in (xn, yn):
        qkv_part(owner)
    for owner, r in pt_owners:
        for k in range(items):
            if k != 2:
                arrived(owner, k, r)
        qkv_part(owner)
    for k in (3, 4, 5, near, near + 1):
        from_diag(k)
    qkv_part(diag)
    for k in range(items):
        if k != 2:
            arrived(last_owner, k, 7)
    qkv_part(last_owner)

    up_rows = U[...].astype(F32).reshape(rank2, heads_width)
    in_query = lax.broadcasted_iota(jnp.int32, (rank2, heads_width), 0) < rank2 // 2
    up_query = jnp.where(in_query, up_rows, 0.0).astype(BF16)
    up_value = jnp.where(in_query, 0.0, up_rows).astype(BF16)
    low = LOW[...].astype(BF16)
    RAW[:, :heads_width] += dot_nn(low, up_query)
    RAW[:, 2 * heads_width :] += dot_nn(low, up_value)

    def head(h, section=0):
        lo = section * heads_width + h * HEAD_SIZE
        return slice(lo, lo + HEAD_SIZE)

    def inverse_of(raw):
        return lax.rsqrt(jnp.mean(raw * raw, -1, keepdims=True) + EPSILON)

    for section in range(3):
        for h in range(nh):
            raw = RAW[:, head(h, section)]
            if section < 2:
                raw = raw * inverse_of(raw)
            QS[:, :, head(h, section)] = to_place(raw.astype(BF16)).reshape(nctx, part, HEAD_SIZE)
    QR[mz] = QS[mz]
    qkv_copies = exchange(QS, QR, qs_sem, qr_sem)
    for copy in grad_copies:
        copy.wait()
    for copy in qkv_copies:
        copy.wait()

    scale = HEAD_SIZE ** (-0.5)

    def whole(ref, where):
        return ref[:, :, where].reshape(rows, HEAD_SIZE)

    weights = []
    for h in range(nh):
        q, k = whole(QR, head(h)), whole(QR, head(h, 1))
        v = whole(QR, head(h, 2))
        expo = jnp.exp(times_transposed(q, k) * scale) * same
        a = expo / jnp.sum(expo, -1, keepdims=True)
        OS[:, :, head(h)] = dot_nn(a.astype(BF16), v).astype(BF16).reshape(nctx, part, HEAD_SIZE)
        weights.append(a)
    OR[mz] = OS[mz]
    out_copies = exchange(OS, OR, os_sem, or_sem)
    for h in range(nh):
        q, k = whole(QR, head(h)), whole(QR, head(h, 1))
        v, g = whole(QR, head(h, 2)), whole(DR, head(h))
        a = weights[h]
        dv = transposed_times(a.astype(BF16), g)
        dp = times_transposed(g, v)
        ds = (a * (dp - jnp.sum(a * dp, -1, keepdims=True)) * scale).astype(BF16)
        dq = dot_nn(ds, k)
        dk = transposed_times(ds, q)
        for section, value in enumerate((dq, dk, dv)):
            GS[:, :, head(h, section)] = value.astype(BF16).reshape(nctx, part, HEAD_SIZE)
    GR[mz] = GS[mz]
    back_copies = exchange(GS, GR, bs_sem, br_sem)

    grad_scale = total_tokens ** (-0.5)
    for copy in out_copies:
        copy.wait()
    OS[...] = to_frame(OR[...].reshape(rows, heads_width)).reshape(nctx, part, heads_width)

    def out_body(j, _):
        branch = dot_nn(OS[...].reshape(rows, heads_width), O[j])
        up = outgrad[:, cols(j)].astype(F32)
        mixed_out[:, cols(j)] = (
            tokens[:, cols(j)].astype(F32) + modulation[2, :, cols(j)] * branch
        ).astype(BF16)
        ZM[mz, 2, pl.ds(j, 1), :] = jnp.sum(up * branch, 0, keepdims=True) * grad_scale
        return 0

    lax.fori_loop(0, ndp, out_body, 0)

    for copy in back_copies:
        copy.wait()
    for section in range(3):
        for h in range(nh):
            where = head(h, section)
            u = to_frame(whole(GR, where))
            if section < 2:
                raw = RAW[:, where]
                inv = inverse_of(raw)
                uf = u.astype(F32)
                inner = jnp.mean(raw * uf, -1, keepdims=True)
                u = (inv * uf - raw * (inv * inv * inv) * inner).astype(BF16)
            JG[:, where] = u
    jq, jv = JG[:, :heads_width], JG[:, 2 * heads_width :]
    LG[...] = (times_transposed(jq, up_query) + times_transposed(jv, up_value)).astype(BF16)
    up_part = jnp.where(in_query, transposed_times(low, jq), transposed_times(low, jv)) * grad_scale
    US[...] = up_part.reshape(ndp, rank2 // ndp, heads_width)

    def down_body(j, _):
        RS[j] = (transposed_times(LG[...], H[j]) * grad_scale).astype(BF16)
        return 0

    lax.fori_loop(0, ndp, down_body, 0)
    reduce_copies = []
    for t in range(1, ndp):
        to = lax.rem(me + t, ndp)
        for src, dst, ss, rs in ((RS, RR, rs_sem, rr_sem), (US, UR, us_sem, ur_sem)):
            copy = pltpu.make_async_remote_copy(
                src_ref=src.at[to], dst_ref=dst.at[t], send_sem=ss.at[t], recv_sem=rs.at[t],
                device_id={"dp": to}, device_id_type=pl.DeviceIdType.MESH)
            copy.start()
            reduce_copies.append(copy)

    def hidden_body(j, sums):
        first, second = sums
        hg = times_transposed(JG[...], W[j]) + dot_nn(LG[...], DT[j])
        n = N[j]
        ZM[mz, 0, pl.ds(j, 1), :] = jnp.sum(hg, 0, keepdims=True) * grad_scale
        ZM[mz, 1, pl.ds(j, 1), :] = jnp.sum(hg * n, 0, keepdims=True) * grad_scale
        ng = hg * (1.0 + modulation[1, :, cols(j)])
        HG[j] = ng
        return (
            first + jnp.sum(ng, -1, keepdims=True),
            second + jnp.sum(ng * n, -1, keepdims=True),
        )

    zero = jnp.zeros((rows, 1), F32)
    first, second = lax.fori_loop(0, ndp, hidden_body, (zero, zero))
    z_copies = []

    def share(ref, row):
        for t in range(1, nctx):
            copy = ctx_copy(ref.at[mz], ref.at[mz], zs_sem.at[row], zr_sem.at[row], t)
            copy.start()
            z_copies.append(copy)

    share(ZM, 0)
    for copy in reduce_copies:
        copy.wait()
    down_sum = RS[me].astype(F32)
    up_sum = US[me]
    for t in range(1, ndp):
        down_sum = down_sum + RR[t].astype(F32)
        up_sum = up_sum + UR[t]
    ZD[mz] = down_sum.astype(BF16)
    ZU[mz] = up_sum
    share(ZD, 1)
    share(ZU, 2)

    first, second = first / width, second / width

    def last_body(j, _):
        grad = outgrad[:, cols(j)].astype(F32) + rstd * (HG[j] - first - N[j] * second)
        tokens_grad[:, cols(j)] = grad.astype(BF16)
        return 0

    lax.fori_loop(0, ndp, last_body, 0)
    for copy in z_copies:
        copy.wait()
    down_all, up_all, mod_all = ZD[0].astype(F32), ZU[0], ZM[0]
    for z in range(1, nctx):
        down_all = down_all + ZD[z].astype(F32)
        up_all = up_all + ZU[z]
        mod_all = mod_all + ZM[z]
    down_out[...] = down_all
    up_out[...] = up_all
    for j in range(ndp):
        for i in range(3):
            mod_out[i, :, j * block : (j + 1) * block] = mod_all[i, j : j + 1, :]

    for k in range(items):
        used = range(10) if k < 2 else range(7) if k < near else (2, 4, 5, 6)
        for s in used:
            push(piece(me, k), me, k, pt, s, 1).wait_send()


def finish_kernel(*refs):
    sem = refs[10]
    copies = [pltpu.make_async_copy(refs[i], refs[5 + i], sem.at[i]) for i in range(5)]
    for copy in copies:
        copy.start()
    for copy in copies:
        copy.wait()


def per_device_kernel(mesh_shape, *args):
    ndp, nctx = mesh_shape
    tokens, modulation, qkv, out, down, up, outgrad = args
    _, frames, places, width = tokens.shape
    rows = frames * places
    block = width // ndp
    rank2 = down.shape[1]
    hw = up.shape[1]
    part = rows // nctx
    dims = (ndp, nctx, rows, places, width, block, hw, rank2, ndp * nctx * rows)
    vm = pl.BlockSpec(memory_space=pltpu.VMEM)
    hbm = pl.BlockSpec(memory_space=pltpu.HBM)
    sem = pltpu.SemaphoreType.DMA
    ur = rank2 // ndp
    scratch = [
        pltpu.VMEM((rows, width), BF16),
        pltpu.VMEM((3, 1, width), F32),
        pltpu.VMEM((rows, width), BF16),
        pltpu.VMEM((ndp, block, 3 * hw), BF16),
        pltpu.VMEM((ndp, hw, block), BF16),
        pltpu.VMEM((ndp, rank2, block), BF16),
        pltpu.VMEM((ndp, ur, hw), BF16),
        pltpu.VMEM((ndp, rows, block), BF16),
        pltpu.VMEM((ndp, rows, block), F32),
        pltpu.VMEM((ndp, rows, block), BF16),
        pltpu.VMEM((rows, 3 * hw), F32),
    ]
    for w in (hw, 3 * hw, hw, 3 * hw):
        scratch += [pltpu.VMEM((nctx, part, w), BF16)] * 2
    scratch += [
        pltpu.VMEM((rows, hw), F32),
        pltpu.VMEM((rows, rank2), F32),
        pltpu.VMEM((rows, 3 * hw), BF16),
        pltpu.VMEM((rows, rank2), BF16),
        pltpu.VMEM((ndp, rows, block), F32),
        pltpu.VMEM((ndp, rank2, block), BF16),
        pltpu.VMEM((ndp, rank2, block), BF16),
        pltpu.VMEM((ndp, ur, hw), F32),
        pltpu.VMEM((ndp, ur, hw), F32),
        pltpu.VMEM((nctx, rank2, block), BF16),
        pltpu.VMEM((nctx, ur, hw), F32),
        pltpu.VMEM((nctx, 3, ndp, block), F32),
        sem((3,)),
        sem((8,)),
        sem((10, 8)),
        sem((8, 8)),
    ]
    scratch += [sem((nctx,))] * 8 + [sem((ndp,))] * 4 + [sem((3, nctx))] * 2
    results = pl.pallas_call(
        functools.partial(layer_kernel, dims),
        out_shape=(
            pltpu.VMEM((rows, width), BF16),
            pltpu.VMEM((rows, width), BF16),
            pltpu.VMEM((3, 1, width), F32),
            pltpu.VMEM((rank2, block), F32),
            pltpu.VMEM((ur, hw), F32),
        ),
        in_specs=[hbm] * 7,
        out_specs=[vm] * 5,
        scratch_shapes=scratch,
        compiler_params=pltpu.CompilerParams(
            collective_id=0, has_side_effects=True, vmem_limit_bytes=52 * 1024 * 1024
        ),
    )(
        tokens.reshape(rows, width),
        pltpu.with_memory_space_constraint(modulation.reshape(3, 1, width), pltpu.HBM),
        outgrad.reshape(rows, width),
        qkv,
        out,
        pltpu.with_memory_space_constraint(down.T, pltpu.HBM),
        pltpu.with_memory_space_constraint(up, pltpu.HBM),
    )
    mixed, tgrad, mod, dgrad, ugrad = pl.pallas_call(
        finish_kernel,
        out_shape=(
            jax.ShapeDtypeStruct((rows, width), BF16),
            jax.ShapeDtypeStruct((rows, width), BF16),
            jax.ShapeDtypeStruct((3, 1, width), F32),
            jax.ShapeDtypeStruct((rank2, block), F32),
            jax.ShapeDtypeStruct((ur, hw), F32),
        ),
        in_specs=[vm] * 5,
        out_specs=[hbm] * 5,
        scratch_shapes=[sem((5,))],
        compiler_params=pltpu.CompilerParams(vmem_limit_bytes=4 * 1024 * 1024),
    )(*results)
    return (
        mixed.reshape(tokens.shape),
        tgrad.reshape(tokens.shape),
        mod.reshape(1, 3, width),
        dgrad.T,
        ugrad,
    )


def solution(mesh):
    ndp, nctx = mesh.shape["dp"], mesh.shape["ctx"]
    body = functools.partial(per_device_kernel, (ndp, nctx)) if ndp == 8 and nctx % 2 == 0 else per_device
    return jax.shard_map(
        body,
        mesh=mesh,
        in_specs=(
            P("dp", "ctx", None, None),
            P("dp", None, None),
            P("dp", None),
            P(None, "dp"),
            P("dp", None),
            P("dp", None),
            P("dp", "ctx", None, None),
        ),
        out_specs=(
            P("dp", "ctx", None, None),
            P("dp", "ctx", None, None),
            P("dp", None, None),
            P("dp", None),
            P("dp", None),
        ),
        check_vma=False,
    )
```

```python
import functools

import jax
import jax.numpy as jnp
from jax import lax
from jax.experimental import pallas as pl
from jax.experimental.pallas import tpu as pltpu
from jax.sharding import PartitionSpec as P

HEAD_SIZE = 128


EPSILON = 1e-06


def times_transposed(left, right):
    return lax.dot_general(
        left, right, (((1,), (1,)), ((), ())), preferred_element_type=jnp.float32
    )


def transposed_times(left, right):
    return lax.dot_general(
        left, right, (((0,), (0,)), ((), ())), preferred_element_type=jnp.float32
    )


def normalize_rows(flat_tokens, modulation_per_clip):
    values = flat_tokens.astype(jnp.float32)
    center = values - jnp.mean(values, -1, keepdims=True)
    inverse_value = lax.rsqrt(jnp.mean(center * center, -1, keepdims=True) + EPSILON)
    normalized_input = center * inverse_value
    hidden_state = (
        normalized_input * (1.0 + modulation_per_clip[1]) + modulation_per_clip[0]
    ).astype(jnp.bfloat16)
    return (normalized_input, inverse_value, hidden_state)


def projection_forward(hidden_state, qkv_full, down_full, up_full, adapter_inner_rank):
    head_size_value = up_full.shape[1]
    base_proj = jnp.dot(hidden_state, qkv_full, preferred_element_type=jnp.float32)
    low_rank_product = jnp.dot(hidden_state, down_full, preferred_element_type=jnp.float32).astype(
        jnp.bfloat16
    )
    delta_query = jnp.dot(
        low_rank_product[:, :adapter_inner_rank],
        up_full[:adapter_inner_rank],
        preferred_element_type=jnp.float32,
    )
    delta_value = jnp.dot(
        low_rank_product[:, adapter_inner_rank:],
        up_full[adapter_inner_rank:],
        preferred_element_type=jnp.float32,
    )
    query_unnormalized = base_proj[:, :head_size_value] + delta_query
    key_unnormalized = base_proj[:, head_size_value : 2 * head_size_value]
    value_row_matrix = (base_proj[:, 2 * head_size_value :] + delta_value).astype(jnp.bfloat16)
    return (low_rank_product, query_unnormalized, key_unnormalized, value_row_matrix)


def head_stats(raw_rows, head_dim):
    grouped = raw_rows.reshape(raw_rows.shape[0], -1, head_dim)
    inverse_value = lax.rsqrt(jnp.mean(grouped * grouped, -1, keepdims=True) + EPSILON)
    return (grouped, inverse_value)


def head_normed(raw_rows, head_dim):
    grouped, inverse_value = head_stats(raw_rows, head_dim)
    return (grouped * inverse_value).reshape(raw_rows.shape).astype(jnp.bfloat16)


def head_norm_back(raw_rows, incoming_grad, head_dim):
    grouped, inverse_value = head_stats(raw_rows, head_dim)
    incoming = incoming_grad.astype(jnp.float32).reshape(grouped.shape)
    inner_mean = jnp.mean(grouped * incoming, -1, keepdims=True)
    return (inverse_value * incoming - grouped * inverse_value**3 * inner_mean).reshape(
        raw_rows.shape
    )


def split_heads(rows_in, head_dim):
    frame_count, place_count, head_size_value = rows_in.shape
    return rows_in.reshape(frame_count, place_count, head_size_value // head_dim, head_dim)


def attend(query_rows, key_rows, value_row_matrix, head_dim):
    score_scale = head_dim ** (-0.5)
    query_heads = split_heads(query_rows, head_dim)
    key_heads = split_heads(key_rows, head_dim)
    value_heads = split_heads(value_row_matrix, head_dim)
    scores = (
        jnp.einsum("fphd,gphd->phfg", query_heads, key_heads, preferred_element_type=jnp.float32)
        * score_scale
    )
    expo = jnp.exp(scores)
    attention_weights = expo / jnp.sum(expo, -1, keepdims=True)
    weights_low = attention_weights.astype(jnp.bfloat16)
    attended = jnp.einsum(
        "phfg,gphd->fphd", weights_low, value_heads, preferred_element_type=jnp.float32
    ).astype(jnp.bfloat16)
    return (attended.reshape(query_rows.shape), attention_weights)


def attend_back(attended_grad, attention_weights, query_rows, key_rows, value_row_matrix, head_dim):
    score_scale = head_dim ** (-0.5)
    grad_heads = split_heads(attended_grad, head_dim)
    query_heads = split_heads(query_rows, head_dim)
    key_heads = split_heads(key_rows, head_dim)
    value_heads = split_heads(value_row_matrix, head_dim)
    weights_low = attention_weights.astype(jnp.bfloat16)
    prob_grad = jnp.einsum(
        "fphd,gphd->phfg", grad_heads, value_heads, preferred_element_type=jnp.float32
    )
    value_gradient = jnp.einsum(
        "phfg,fphd->gphd", weights_low, grad_heads, preferred_element_type=jnp.float32
    ).astype(jnp.bfloat16)
    score_grad = attention_weights * (
        prob_grad - jnp.sum(attention_weights * prob_grad, -1, keepdims=True)
    )
    score_low = (score_grad * score_scale).astype(jnp.bfloat16)
    query_grad = jnp.einsum(
        "phfg,gphd->fphd", score_low, key_heads, preferred_element_type=jnp.float32
    ).astype(jnp.bfloat16)
    key_grad = jnp.einsum(
        "phfg,fphd->gphd", score_low, query_heads, preferred_element_type=jnp.float32
    ).astype(jnp.bfloat16)
    shape_rows = query_rows.shape
    return (
        query_grad.reshape(shape_rows),
        key_grad.reshape(shape_rows),
        value_gradient.reshape(shape_rows),
    )


def projection_backward(
    query_normalized_gradient,
    key_normalized_gradient,
    value_gradient,
    query_unnormalized,
    key_unnormalized,
    hidden_state,
    low_rank_product,
    normalized_input,
    inverse_value,
    modulation_per_clip,
    qkv_full,
    down_full,
    up_full,
    adapter_inner_rank,
    head_dim,
):
    head_size_value = up_full.shape[1]
    query_back = head_norm_back(query_unnormalized, query_normalized_gradient, head_dim)
    key_back = head_norm_back(key_unnormalized, key_normalized_gradient, head_dim)
    joined_grad = jnp.concatenate(
        [query_back, key_back, value_gradient.astype(jnp.float32)], 1
    ).astype(jnp.bfloat16)
    query_block = joined_grad[:, :head_size_value]
    value_block = joined_grad[:, 2 * head_size_value :]
    up_grad = jnp.concatenate(
        [
            transposed_times(low_rank_product[:, :adapter_inner_rank], query_block),
            transposed_times(low_rank_product[:, adapter_inner_rank:], value_block),
        ],
        0,
    )
    low_grad = jnp.concatenate(
        [
            times_transposed(query_block, up_full[:adapter_inner_rank]),
            times_transposed(value_block, up_full[adapter_inner_rank:]),
        ],
        1,
    ).astype(jnp.bfloat16)
    hidden_grad = times_transposed(joined_grad, qkv_full) + times_transposed(low_grad, down_full)
    down_grad = transposed_times(hidden_state, low_grad)
    shift_gradient = jnp.sum(hidden_grad, 0)
    scale_gradient = jnp.sum(hidden_grad * normalized_input, 0)
    normed_grad = hidden_grad * (1.0 + modulation_per_clip[1])
    first_mean = jnp.mean(normed_grad, -1, keepdims=True)
    second_mean = jnp.mean(normed_grad * normalized_input, -1, keepdims=True)
    token_gradient_rows = inverse_value * (
        normed_grad - first_mean - normalized_input * second_mean
    )
    return (token_gradient_rows, shift_gradient, scale_gradient, down_grad, up_grad)


def per_device(
    tokens,
    modulation,
    query_key_value_weight,
    output_projection_weight,
    adapter_down_maps,
    adapter_up_maps,
    output_gradient,
):
    adapter_inner_rank = adapter_down_maps.shape[1] // 2
    head_dim = HEAD_SIZE
    qkv_full, out_full, down_full, up_full = (
        lax.all_gather(query_key_value_weight, "dp", axis=0, tiled=True),
        lax.all_gather(output_projection_weight, "dp", axis=1, tiled=True),
        lax.all_gather(adapter_down_maps, "dp", axis=0, tiled=True),
        lax.all_gather(adapter_up_maps, "dp", axis=0, tiled=True),
    )
    head_size_value = up_full.shape[1]
    local_shape = tokens.shape
    frame_shape = (1, local_shape[1], local_shape[2], head_size_value)
    modulation_per_clip = modulation[0]
    flat_tokens = tokens.reshape(-1, local_shape[3])
    normalized_input, inverse_value, hidden_state = normalize_rows(flat_tokens, modulation_per_clip)
    low_rank_product, query_unnormalized, key_unnormalized, value_row_matrix = projection_forward(
        hidden_state, qkv_full, down_full, up_full, adapter_inner_rank
    )
    query_rows = head_normed(query_unnormalized, head_dim)
    key_rows = head_normed(key_unnormalized, head_dim)
    upstream = output_gradient.reshape(-1, local_shape[3]).astype(jnp.float32)
    branch_grad = (upstream * modulation_per_clip[2]).astype(jnp.bfloat16)
    attended_grad = (
        times_transposed(branch_grad, out_full).astype(jnp.bfloat16).reshape(frame_shape)
    )
    query_place, key_place, value_place = (
        lax.all_to_all(
            query_rows.reshape(frame_shape), "ctx", split_axis=2, concat_axis=1, tiled=True
        ),
        lax.all_to_all(
            key_rows.reshape(frame_shape), "ctx", split_axis=2, concat_axis=1, tiled=True
        ),
        lax.all_to_all(
            value_row_matrix.reshape(frame_shape), "ctx", split_axis=2, concat_axis=1, tiled=True
        ),
    )
    attended, attention_weights = attend(query_place[0], key_place[0], value_place[0], head_dim)
    attended_frames = lax.all_to_all(attended[None], "ctx", split_axis=1, concat_axis=2, tiled=True)
    grad_place = lax.all_to_all(attended_grad, "ctx", split_axis=2, concat_axis=1, tiled=True)
    query_normalized_gradient, key_normalized_gradient, value_gradient = attend_back(
        grad_place[0], attention_weights, query_place[0], key_place[0], value_place[0], head_dim
    )
    query_back_frames, key_back_frames, value_back_frames = (
        lax.all_to_all(
            query_normalized_gradient[None], "ctx", split_axis=1, concat_axis=2, tiled=True
        ),
        lax.all_to_all(
            key_normalized_gradient[None], "ctx", split_axis=1, concat_axis=2, tiled=True
        ),
        lax.all_to_all(value_gradient[None], "ctx", split_axis=1, concat_axis=2, tiled=True),
    )
    branch_out = jnp.dot(
        attended_frames.reshape(-1, head_size_value), out_full, preferred_element_type=jnp.float32
    )
    mixed_out = (flat_tokens.astype(jnp.float32) + modulation_per_clip[2] * branch_out).astype(
        jnp.bfloat16
    )
    gate_grad = jnp.sum(upstream * branch_out, 0)
    token_gradient_rows, shift_gradient, scale_gradient, down_section, up_section = (
        projection_backward(
            query_back_frames.reshape(-1, head_size_value),
            key_back_frames.reshape(-1, head_size_value),
            value_back_frames.reshape(-1, head_size_value),
            query_unnormalized,
            key_unnormalized,
            hidden_state,
            low_rank_product,
            normalized_input,
            inverse_value,
            modulation_per_clip,
            qkv_full,
            down_full,
            up_full,
            adapter_inner_rank,
            head_dim,
        )
    )
    tokens_grad = (upstream + token_gradient_rows).astype(jnp.bfloat16)
    token_total = lax.axis_size("dp") * lax.axis_size("ctx") * flat_tokens.shape[0]
    grad_scale = token_total ** (-0.5)
    modulation_part = jnp.stack([shift_gradient, scale_gradient, gate_grad], 0)[None] * grad_scale
    down_section = down_section * grad_scale
    up_section = up_section * grad_scale
    down_total, up_total, modulation_grad = (
        lax.psum(down_section.astype(jnp.bfloat16), "ctx").astype(jnp.float32),
        lax.psum(up_section.astype(jnp.bfloat16), "ctx").astype(jnp.float32),
        lax.psum(modulation_part.astype(jnp.bfloat16), "ctx").astype(jnp.float32),
    )
    down_grad, up_grad = (
        lax.psum_scatter(
            down_total.astype(jnp.bfloat16), "dp", scatter_dimension=0, tiled=True
        ).astype(jnp.float32),
        lax.psum_scatter(
            up_total.astype(jnp.bfloat16), "dp", scatter_dimension=0, tiled=True
        ).astype(jnp.float32),
    )
    return (
        mixed_out.reshape(local_shape),
        tokens_grad.reshape(local_shape),
        modulation_grad,
        down_grad,
        up_grad,
    )


BF16 = jnp.bfloat16
F32 = jnp.float32


def dot_nn(a, b):
    return lax.dot_general(a, b, (((1,), (0,)), ((), ())), preferred_element_type=F32)


GROUPS = 2
SHARED_ROWS = 16


def place(y, x, c):
    return y * 4 + x * 2 + c


def layer_kernel(
    dims,
    tokens_in, modulation_in, outgrad_in, qkv_in, out_in, down_in, up_in,
    mixed_out, tokens_grad, mod_out, down_out, up_out,
    tokens, modulation, outgrad, W, O, DT, U, H, N, BG, RAW, DS, DR, QS, QR, OS, OR, GS, GR,
    WT, LOW, LT, JG, LG, LGT, HG, AW, OF, RS, RR, US, UR, ZD, ZU, ZM, ZL,
    load_sem, local_sem, gs_sem, gr_sem, ds_sem, dr_sem, qs_sem, qr_sem, os_sem, or_sem,
    bs_sem, br_sem, rs_sem, rr_sem, us_sem, ur_sem, zs_sem, zr_sem,
):
    ndp, nctx, rows, places, width, block, heads_width, rank2, total_tokens = dims
    nh = heads_width // HEAD_SIZE
    part = rows // nctx
    gw = heads_width // GROUPS
    per_group = nh // GROUPS
    me = lax.axis_index("dp")
    mz = lax.axis_index("ctx")
    y, x, c = me // 4, (me // 2) % 2, me % 2
    y1, x1, c1 = 1 - y, 1 - x, 1 - c
    xn, yn, pt = place(y, x1, c), place(y1, x, c), place(y, x, c1)
    rel_owner = place((y + c) % 2, (x + 1 - c) % 2, c)
    rel_target = place((y + 1 - c) % 2, (x + c) % 2, c)
    oth_owner = rel_target
    diag = place(y1, x1, c)
    rel_r = 2 + 2 * c
    oth_r = 4 - 2 * c

    barrier = pltpu.get_barrier_semaphore()
    for t in range(1, ndp):
        pl.semaphore_signal(barrier, inc=1, device_id={"dp": lax.rem(me + t, ndp)}, device_id_type=pl.DeviceIdType.MESH)
    for t in range(1, nctx):
        pl.semaphore_signal(barrier, inc=1, device_id={"ctx": lax.rem(mz + t, nctx)}, device_id_type=pl.DeviceIdType.MESH)

    parity = mz % 2
    pair_z = mz + 1 - 2 * parity
    big = block // 48 * SHARED_ROWS
    rest = block - 2 * big
    NEAR, REST, FAR = (0, 3), (1, 4), (2, 5)
    DOWN, UP = 6, 7
    OUT = tuple(range(8, 8 + nh))
    items = 8 + nh

    def piece(owner, k):
        if k in OUT:
            return O.at[owner, pl.ds((k - OUT[0]) * HEAD_SIZE, HEAD_SIZE), :]
        if k == DOWN:
            return DT.at[owner]
        if k == UP:
            return U.at[owner]
        if k in REST:
            span = pl.ds(0, rest)
        else:
            side = parity if k in NEAR else 1 - parity
            span = pl.ds(pl.multiple_of(rest + side * big, 16), big)
        return W.at[owner, k // 3, span, :]

    def push(owner, k, target, s, r):
        return pltpu.make_async_remote_copy(
            src_ref=piece(owner, k), dst_ref=piece(owner, k), send_sem=gs_sem.at[s, k],
            recv_sem=gr_sem.at[r, k],
            device_id={"dp": target}, device_id_type=pl.DeviceIdType.MESH)

    def across(owner, k, s, r):
        pltpu.make_async_remote_copy(
            src_ref=piece(owner, k), dst_ref=piece(owner, k), send_sem=gs_sem.at[s, k],
            recv_sem=gr_sem.at[r, k + 2],
            device_id={"ctx": pair_z}, device_id_type=pl.DeviceIdType.MESH).start()

    def arrived(owner, k, r):
        push(owner, k, pt, 0, r).wait_recv()

    def forward(owner, k, s, r):
        push(owner, k, pt, s, r).start()

    def own_out(k):
        push(me, k, xn, 0, 2).start()
        push(me, k, yn, 1, 4).start()

    def from_sides(k):
        arrived(rel_owner, k, rel_r)
        push(rel_owner, k, rel_target, 3, 6).start()
        if k in NEAR:
            across(rel_owner, k, 7, rel_r)
        forward(rel_owner, k, 4, 1 + rel_r)
        arrived(oth_owner, k, oth_r)
        if k in NEAR:
            across(oth_owner, k, 8, oth_r)
        forward(oth_owner, k, 5, 1 + oth_r)

    def from_diag(k):
        arrived(diag, k, 6)
        if k in NEAR:
            across(diag, k, 9, 6)
        forward(diag, k, 6, 7)

    def from_far(k):
        arrived(rel_owner, k, rel_r)
        forward(rel_owner, k, 4, 1 + rel_r)
        arrived(oth_owner, k, oth_r)
        forward(oth_owner, k, 5, 1 + oth_r)

    locals_ = []
    for g in range(GROUPS):
        for section in range(3):
            locals_.append(pltpu.make_async_copy(
                qkv_in.at[:, pl.ds(section * heads_width + g * gw, gw)],
                W.at[me, g, :, pl.ds(section * gw, gw)],
                local_sem.at[3 * g + section]))
    locals_.append(pltpu.make_async_copy(down_in, DT.at[me], local_sem.at[6]))
    locals_.append(pltpu.make_async_copy(up_in, U.at[me], local_sem.at[7]))
    locals_.append(pltpu.make_async_copy(out_in, O.at[me], local_sem.at[8]))
    for copy in locals_:
        copy.start()
    loads = []
    for t, (src, dst) in enumerate(((tokens_in, tokens), (outgrad_in, outgrad), (modulation_in, modulation))):
        load = pltpu.make_async_copy(src, dst, load_sem.at[t])
        load.start()
        loads.append(load)
    for copy in locals_[:3]:
        copy.wait()
    pl.semaphore_wait(barrier, ndp - 1 + nctx - 1)
    own_out(NEAR[0])
    for copy in locals_[3:]:
        copy.wait()
    own_out(DOWN)
    own_out(UP)
    own_out(REST[0])
    for k in (0, 1, 2, 6, 7, 3, 4, 5) + OUT:
        push(me, k, pt, 2, 1).start()
    for load in loads:
        load.wait()

    def cols(j):
        return pl.ds(pl.multiple_of(j * block, 128), block)

    def sum_body(j, s):
        return s + jnp.sum(tokens[:, cols(j)].astype(F32), -1, keepdims=True)

    mean = lax.fori_loop(0, ndp, sum_body, jnp.zeros((rows, 1), F32)) / width

    def var_body(j, s):
        d = tokens[:, cols(j)].astype(F32) - mean
        return s + jnp.sum(d * d, -1, keepdims=True)

    var = lax.fori_loop(0, ndp, var_body, jnp.zeros((rows, 1), F32)) / width
    rstd = lax.rsqrt(var + EPSILON)

    def norm_body(j, _):
        n = (tokens[:, cols(j)].astype(F32) - mean) * rstd
        N[j] = n
        H[j] = (n * (1.0 + modulation[1, :, cols(j)]) + modulation[0, :, cols(j)]).astype(BF16)
        BG[j] = (outgrad[:, cols(j)].astype(F32) * modulation[2, :, cols(j)]).astype(BF16)
        return 0

    lax.fori_loop(0, ndp, norm_body, 0)

    far_side = place(y, x1, c1), place(y1, x, c1), place(y1, x1, c1)
    pt_owners = ((pt, 1), (far_side[0], 3), (far_side[1], 5))
    last_owner = far_side[2]

    def grad_part(owner, g):
        WT[g] += times_transposed(BG[owner], O[owner, g * gw : (g + 1) * gw, :])

    def qkv_part(owner, g):
        RAW[g] += dot_nn(H[owner], W[owner, g])

    def low_part(owner):
        LOW[...] += times_transposed(H[owner], DT[owner])

    def got(owner, r, kinds):
        for k in kinds:
            arrived(owner, k, r)

    frames = rows // places
    across_rows = lax.broadcasted_iota(jnp.int32, (rows, rows), 0)
    along_rows = lax.broadcasted_iota(jnp.int32, (rows, rows), 1)
    perm = jnp.where(
        along_rows == (across_rows % frames) * places + across_rows // frames, 1.0, 0.0
    ).astype(BF16)
    perm_back = jnp.where(
        across_rows == (along_rows % frames) * places + along_rows // frames, 1.0, 0.0
    ).astype(BF16)
    local_places = places // nctx
    same = jnp.where(
        (across_rows // frames) % local_places == (along_rows // frames) % local_places, 1.0, 0.0
    )

    def to_place(value):
        return dot_nn(perm, value).astype(BF16)

    def to_frame(value):
        return dot_nn(perm_back, value).astype(BF16)

    def ctx_copy(src, dst, ssem, rsem, t):
        return pltpu.make_async_remote_copy(
            src_ref=src, dst_ref=dst, send_sem=ssem, recv_sem=rsem,
            device_id={"ctx": lax.rem(mz + t, nctx)}, device_id_type=pl.DeviceIdType.MESH)

    def exchange(sent, got_ref, ssem, rsem, g):
        copies = []
        got_ref[g, mz] = sent[g, mz]
        for t in range(1, nctx):
            copy = ctx_copy(
                sent.at[g, lax.rem(mz + t, nctx)], got_ref.at[g, mz], ssem.at[g, t], rsem.at[g, t], t)
            copy.start()
            copies.append(copy)
        return copies

    def wait_all(copies):
        for copy in copies:
            copy.wait()

    def lanes(i, section=0):
        lo = section * gw + i * HEAD_SIZE
        return slice(lo, lo + HEAD_SIZE)

    def inverse_of(raw):
        return lax.rsqrt(jnp.mean(raw * raw, -1, keepdims=True) + EPSILON)

    def up_maps():
        up_rows = U[...].astype(F32).reshape(rank2, heads_width)
        in_query = lax.broadcasted_iota(jnp.int32, (rank2, heads_width), 0) < rank2 // 2
        return (
            jnp.where(in_query, up_rows, 0.0).astype(BF16),
            jnp.where(in_query, 0.0, up_rows).astype(BF16),
        )

    def send_qkv(g):
        up_query, up_value = up_maps()
        low = LOW[...].astype(BF16)
        mine = slice(g * gw, (g + 1) * gw)
        RAW[g, :, :gw] += dot_nn(low, up_query[:, mine])
        RAW[g, :, 2 * gw :] += dot_nn(low, up_value[:, mine])
        for section in range(3):
            for i in range(per_group):
                raw = RAW[g, :, lanes(i, section)]
                if section < 2:
                    raw = raw * inverse_of(raw)
                QS[g, :, :, lanes(i, section)] = to_place(raw.astype(BF16)).reshape(nctx, part, HEAD_SIZE)
        return exchange(QS, QR, qs_sem, qr_sem, g)

    def send_grad(h):
        raw = WT[h // per_group, :, lanes(h % per_group)]
        DS[h] = to_place(raw.astype(BF16)).reshape(nctx, part, HEAD_SIZE)
        return exchange(DS, DR, ds_sem, dr_sem, h)

    scale = HEAD_SIZE ** (-0.5)

    def whole(ref, g, where):
        return ref[g, :, :, where].reshape(rows, HEAD_SIZE)

    def attend_group(g):
        for i in range(per_group):
            q, k = whole(QR, g, lanes(i)), whole(QR, g, lanes(i, 1))
            v = whole(QR, g, lanes(i, 2))
            expo = jnp.exp(times_transposed(q, k) * scale) * same
            a = expo / jnp.sum(expo, -1, keepdims=True)
            OS[g, :, :, lanes(i)] = dot_nn(a.astype(BF16), v).astype(BF16).reshape(nctx, part, HEAD_SIZE)
            AW[g * per_group + i] = a
        return exchange(OS, OR, os_sem, or_sem, g)

    def attend_back(h):
        g, i = h // per_group, h % per_group
        q, k = whole(QR, g, lanes(i)), whole(QR, g, lanes(i, 1))
        v, d = whole(QR, g, lanes(i, 2)), whole(DR, h, slice(None))
        a = AW[h]
        dv = transposed_times(a.astype(BF16), d)
        dp = times_transposed(d, v)
        ds = (a * (dp - jnp.sum(a * dp, -1, keepdims=True)) * scale).astype(BF16)
        dq = dot_nn(ds, k)
        dk = transposed_times(ds, q)
        for section, value in enumerate((dq, dk, dv)):
            where = slice(section * HEAD_SIZE, (section + 1) * HEAD_SIZE)
            GS[h, :, :, where] = value.astype(BF16).reshape(nctx, part, HEAD_SIZE)
        return exchange(GS, GR, bs_sem, br_sem, h)

    def norm_back(h):
        g, i = h // per_group, h % per_group
        for section in range(3):
            where = lanes(i, section)
            u = to_frame(whole(GR, h, slice(section * HEAD_SIZE, (section + 1) * HEAD_SIZE)))
            if section < 2:
                raw = RAW[g, :, where]
                inv = inverse_of(raw)
                uf = u.astype(F32)
                inner = jnp.mean(raw * uf, -1, keepdims=True)
                u = (inv * uf - raw * (inv * inv * inv) * inner).astype(BF16)
            JG[g, :, where] = u

    grad_scale = total_tokens ** (-0.5)

    def low_grad_part(g):
        up_query, up_value = up_maps()
        in_query = lax.broadcasted_iota(jnp.int32, (rank2, gw), 0) < rank2 // 2
        mine = slice(g * gw, (g + 1) * gw)
        jq, jv = JG[g, :, :gw], JG[g, :, 2 * gw :]
        low = LT[...]
        up_part = jnp.where(in_query, dot_nn(low, jq), dot_nn(low, jv)) * grad_scale
        US[:, :, mine] = up_part.reshape(ndp, rank2 // ndp, gw).astype(BF16)
        return times_transposed(jq, up_query[:, mine]) + times_transposed(jv, up_value[:, mine])

    RAW[...] = jnp.zeros_like(RAW)
    LOW[...] = jnp.zeros_like(LOW)
    WT[...] = jnp.zeros_like(WT)
    low_part(me)
    for g in range(GROUPS):
        qkv_part(me, g)
        grad_part(me, g)

    from_sides(NEAR[0])
    from_sides(DOWN)
    from_sides(UP)
    from_sides(REST[0])
    own_out(NEAR[1])
    own_out(REST[1])
    got(pt, 1, (0, 1, 2, DOWN, UP))
    low_part(pt)
    qkv_part(pt, 0)
    from_diag(NEAR[0])
    from_diag(DOWN)
    from_diag(UP)
    from_far(FAR[0])
    from_diag(REST[0])
    for owner in (xn, yn):
        low_part(owner)
        qkv_part(owner, 0)
    low_part(diag)
    for owner, r in pt_owners[1:]:
        got(owner, r, (0, 1, 2, DOWN, UP))
        low_part(owner)
        qkv_part(owner, 0)
    from_sides(NEAR[1])
    from_diag(FAR[0])
    qkv_part(diag, 0)
    got(last_owner, 7, (0, 1, 2, DOWN, UP))
    low_part(last_owner)
    qkv_part(last_owner, 0)
    qkv_copies = [send_qkv(0)]
    LT[...] = LOW[...].T.astype(BF16)

    from_sides(REST[1])
    early, late = OUT[:per_group], OUT[per_group:]
    for k in early:
        own_out(k)
    got(pt, 1, (3, 4, 5))
    qkv_part(pt, 1)
    from_diag(NEAR[1])
    own_out(late[0])
    from_far(FAR[1])
    from_diag(REST[1])
    for owner in (xn, yn):
        qkv_part(owner, 1)
    for k in early:
        from_sides(k)
    for k in late[1:]:
        own_out(k)
    wait_all(qkv_copies[0])
    out_copies = [attend_group(0)]
    for owner, r in pt_owners[1:]:
        got(owner, r, (3, 4, 5))
        qkv_part(owner, 1)
    from_diag(FAR[1])
    qkv_part(diag, 1)
    from_sides(late[0])
    got(last_owner, 7, (3, 4, 5))
    qkv_part(last_owner, 1)
    qkv_copies.append(send_qkv(1))

    def start_grad(g, keys):
        for owner in (xn, yn, diag):
            grad_part(owner, g)
        for owner, r in pt_owners:
            got(owner, r, keys)
            grad_part(owner, g)

    def finish_grad(g, keys):
        got(last_owner, 7, keys)
        grad_part(last_owner, g)
        return [send_grad(h) for h in range(g * per_group, (g + 1) * per_group)]

    for k in early:
        from_diag(k)
    for k in late[1:]:
        from_sides(k)
    start_grad(0, early)
    grad_copies = finish_grad(0, early)
    for k in late:
        from_diag(k)
    start_grad(1, late)
    grad_copies += finish_grad(1, late)
    back_copies = []
    for h in range(per_group):
        wait_all(grad_copies[h])
        back_copies.append(attend_back(h))
    wait_all(qkv_copies[1])
    out_copies.append(attend_group(1))
    for h in range(per_group, nh):
        wait_all(grad_copies[h])
        back_copies.append(attend_back(h))

    z_copies = []

    def share(view, row):
        for t in range(1, nctx):
            copy = ctx_copy(view, view, zs_sem.at[row, t], zr_sem.at[row, t], t)
            copy.start()
            z_copies.append(copy)

    for h in range(per_group):
        wait_all(back_copies[h])
        norm_back(h)

    def first_hidden(j, _):
        HG[j] = times_transposed(JG[0], W[j, 0])
        return 0

    lax.fori_loop(0, ndp, first_hidden, 0)
    low_grad = low_grad_part(0)
    for g in range(GROUPS):
        wait_all(out_copies[g])
        OF[:, g * gw : (g + 1) * gw] = to_frame(OR[g].reshape(rows, gw))

    def out_body(j, _):
        branch = dot_nn(OF[...], O[j])
        up = outgrad[:, cols(j)].astype(F32)
        mixed_out[:, cols(j)] = (
            tokens[:, cols(j)].astype(F32) + modulation[2, :, cols(j)] * branch
        ).astype(BF16)
        ZL[2, pl.ds(j, 1), :] = jnp.sum(up * branch, 0, keepdims=True) * grad_scale
        return 0

    lax.fori_loop(0, ndp, out_body, 0)
    ZM[mz, 2] = ZL[2].astype(BF16)
    for h in range(per_group, nh):
        wait_all(back_copies[h])
        norm_back(h)
    share(ZM.at[mz, 2], 0)
    low_grad = low_grad + low_grad_part(1)
    LG[...] = low_grad.astype(BF16)
    LGT[...] = low_grad.T.astype(BF16)
    half = rank2 // 2

    def reduce_to(src, dst, ss, rs, to):
        copy = pltpu.make_async_remote_copy(
            src_ref=src, dst_ref=dst, send_sem=ss, recv_sem=rs,
            device_id={"dp": to}, device_id_type=pl.DeviceIdType.MESH)
        copy.start()
        return copy

    def others():
        return [(t, lax.rem(me + t, ndp)) for t in range(1, ndp)]

    up_copies = [
        reduce_to(US.at[to], UR.at[t], us_sem.at[t], ur_sem.at[t], to) for t, to in others()
    ]

    def down_part(j):
        both = (dot_nn(LGT[...], H[j]) * grad_scale).astype(BF16)
        RS[j, 0] = both[:half]
        RS[j, 1] = both[half:]

    def reduce_down(i, t, to):
        return reduce_to(RS.at[to, i], RR.at[t, i], rs_sem.at[i, t], rr_sem.at[i, t], to)

    down_copies = [[], []]
    for t, to in others():
        down_part(to)
        down_copies[0].append(reduce_down(0, t, to))
    for t, to in others():
        down_copies[1].append(reduce_down(1, t, to))
    down_part(me)

    def hidden_body(j, sums):
        first, second = sums
        hg = HG[j] + times_transposed(JG[1], W[j, 1]) + dot_nn(LG[...], DT[j])
        n = N[j]
        ZL[0, pl.ds(j, 1), :] = jnp.sum(hg, 0, keepdims=True) * grad_scale
        ZL[1, pl.ds(j, 1), :] = jnp.sum(hg * n, 0, keepdims=True) * grad_scale
        ng = hg * (1.0 + modulation[1, :, cols(j)])
        HG[j] = ng
        return (
            first + jnp.sum(ng, -1, keepdims=True),
            second + jnp.sum(ng * n, -1, keepdims=True),
        )

    def share_down(i):
        wait_all(down_copies[i])
        total = RS[me, i].astype(F32)
        for t in range(1, ndp):
            total = total + RR[t, i].astype(F32)
        ZD[mz, i] = total.astype(BF16)
        share(ZD.at[mz, i], 2 + i)

    zero = jnp.zeros((rows, 1), F32)
    sums = lax.fori_loop(0, ndp // 2, hidden_body, (zero, zero))
    wait_all(up_copies)
    up_sum = US[me].astype(F32)
    for t in range(1, ndp):
        up_sum = up_sum + UR[t].astype(F32)
    ZU[mz] = up_sum.astype(BF16)
    share(ZU.at[mz], 1)
    first, second = lax.fori_loop(ndp // 2, ndp, hidden_body, sums)
    share_down(0)
    ZM[mz, pl.ds(0, 2)] = ZL[0:2].astype(BF16)
    share(ZM.at[mz, pl.ds(0, 2)], 4)
    first, second = first / width, second / width

    def last_body(j, _):
        grad = outgrad[:, cols(j)].astype(F32) + rstd * (HG[j] - first - N[j] * second)
        tokens_grad[:, cols(j)] = grad.astype(BF16)
        return 0

    lax.fori_loop(0, ndp, last_body, 0)
    share_down(1)
    wait_all(z_copies)
    down_all, up_all, mod_all = ZD[0].astype(F32), ZU[0].astype(F32), ZM[0].astype(F32)
    for z in range(1, nctx):
        down_all = down_all + ZD[z].astype(F32)
        up_all = up_all + ZU[z].astype(F32)
        mod_all = mod_all + ZM[z].astype(F32)
    for i in range(2):
        down_out[i * half : (i + 1) * half, :] = down_all[i]
    up_out[...] = up_all
    for j in range(ndp):
        for i in range(3):
            mod_out[i, :, j * block : (j + 1) * block] = mod_all[i, j : j + 1, :]

    for k in range(items):
        used = range(10) if k in NEAR else (2, 4, 5, 6) if k in FAR else range(7)
        for s in used:
            push(me, k, pt, s, 1).wait_send()


def finish_kernel(*refs):
    sem = refs[10]
    copies = [pltpu.make_async_copy(refs[i], refs[5 + i], sem.at[i]) for i in range(5)]
    for copy in copies:
        copy.start()
    for copy in copies:
        copy.wait()


def per_device_kernel(mesh_shape, *args):
    ndp, nctx = mesh_shape
    tokens, modulation, qkv, out, down, up, outgrad = args
    _, frames, places, width = tokens.shape
    rows = frames * places
    block = width // ndp
    rank2 = down.shape[1]
    hw = up.shape[1]
    part = rows // nctx
    dims = (ndp, nctx, rows, places, width, block, hw, rank2, ndp * nctx * rows)
    vm = pl.BlockSpec(memory_space=pltpu.VMEM)
    hbm = pl.BlockSpec(memory_space=pltpu.HBM)
    sem = pltpu.SemaphoreType.DMA
    ur = rank2 // ndp
    gw = hw // GROUPS
    scratch = [
        pltpu.VMEM((rows, width), BF16),
        pltpu.VMEM((3, 1, width), F32),
        pltpu.VMEM((rows, width), BF16),
        pltpu.VMEM((ndp, GROUPS, block, 3 * gw), BF16),
        pltpu.VMEM((ndp, hw, block), BF16),
        pltpu.VMEM((ndp, rank2, block), BF16),
        pltpu.VMEM((ndp, ur, hw), BF16),
        pltpu.VMEM((ndp, rows, block), BF16),
        pltpu.VMEM((ndp, rows, block), F32),
        pltpu.VMEM((ndp, rows, block), BF16),
        pltpu.VMEM((GROUPS, rows, 3 * gw), F32),
    ]
    nh = hw // HEAD_SIZE
    for n, w in ((nh, HEAD_SIZE), (GROUPS, 3 * gw), (GROUPS, gw), (nh, 3 * HEAD_SIZE)):
        scratch += [pltpu.VMEM((n, nctx, part, w), BF16)] * 2
    scratch += [
        pltpu.VMEM((GROUPS, rows, gw), F32),
        pltpu.VMEM((rows, rank2), F32),
        pltpu.VMEM((rank2, rows), BF16),
        pltpu.VMEM((GROUPS, rows, 3 * gw), BF16),
        pltpu.VMEM((rows, rank2), BF16),
        pltpu.VMEM((rank2, rows), BF16),
        pltpu.VMEM((ndp, rows, block), F32),
        pltpu.VMEM((nh, rows, rows), F32),
        pltpu.VMEM((rows, hw), BF16),
        pltpu.VMEM((ndp, 2, rank2 // 2, block), BF16),
        pltpu.VMEM((ndp, 2, rank2 // 2, block), BF16),
        pltpu.VMEM((ndp, ur, hw), BF16),
        pltpu.VMEM((ndp, ur, hw), BF16),
        pltpu.VMEM((nctx, 2, rank2 // 2, block), BF16),
        pltpu.VMEM((nctx, ur, hw), BF16),
        pltpu.VMEM((nctx, 3, ndp, block), BF16),
        pltpu.VMEM((3, ndp, block), F32),
        sem((3,)),
        sem((9,)),
        sem((10, 8 + nh)),
        sem((8, 8 + nh)),
    ]
    scratch += [sem((nh, nctx))] * 8 + [sem((2, ndp))] * 2 + [sem((ndp,))] * 2 + [sem((5, nctx))] * 2
    results = pl.pallas_call(
        functools.partial(layer_kernel, dims),
        out_shape=(
            pltpu.VMEM((rows, width), BF16),
            pltpu.VMEM((rows, width), BF16),
            pltpu.VMEM((3, 1, width), F32),
            pltpu.VMEM((rank2, block), F32),
            pltpu.VMEM((ur, hw), F32),
        ),
        in_specs=[hbm] * 7,
        out_specs=[vm] * 5,
        scratch_shapes=scratch,
        compiler_params=pltpu.CompilerParams(
            collective_id=0, has_side_effects=True, vmem_limit_bytes=52 * 1024 * 1024
        ),
    )(
        tokens.reshape(rows, width),
        pltpu.with_memory_space_constraint(modulation.reshape(3, 1, width), pltpu.HBM),
        outgrad.reshape(rows, width),
        qkv,
        out,
        pltpu.with_memory_space_constraint(down.T, pltpu.HBM),
        pltpu.with_memory_space_constraint(up, pltpu.HBM),
    )
    mixed, tgrad, mod, dgrad, ugrad = pl.pallas_call(
        finish_kernel,
        out_shape=(
            jax.ShapeDtypeStruct((rows, width), BF16),
            jax.ShapeDtypeStruct((rows, width), BF16),
            jax.ShapeDtypeStruct((3, 1, width), F32),
            jax.ShapeDtypeStruct((rank2, block), F32),
            jax.ShapeDtypeStruct((ur, hw), F32),
        ),
        in_specs=[vm] * 5,
        out_specs=[hbm] * 5,
        scratch_shapes=[sem((5,))],
        compiler_params=pltpu.CompilerParams(vmem_limit_bytes=4 * 1024 * 1024),
    )(*results)
    return (
        mixed.reshape(tokens.shape),
        tgrad.reshape(tokens.shape),
        mod.reshape(1, 3, width),
        dgrad.T,
        ugrad,
    )


def solution(mesh):
    ndp, nctx = mesh.shape["dp"], mesh.shape["ctx"]
    body = functools.partial(per_device_kernel, (ndp, nctx)) if ndp == 8 and nctx % 2 == 0 else per_device
    return jax.shard_map(
        body,
        mesh=mesh,
        in_specs=(
            P("dp", "ctx", None, None),
            P("dp", None, None),
            P("dp", None),
            P(None, "dp"),
            P("dp", None),
            P("dp", None),
            P("dp", "ctx", None, None),
        ),
        out_specs=(
            P("dp", "ctx", None, None),
            P("dp", "ctx", None, None),
            P("dp", None, None),
            P("dp", None),
            P("dp", None),
        ),
        check_vma=False,
    )
```

```python
import functools

import jax
import jax.numpy as jnp
from jax import lax
from jax.experimental import pallas as pl
from jax.experimental.pallas import tpu as pltpu
from jax.sharding import PartitionSpec as P

HEAD_SIZE = 128


EPSILON = 1e-06


def times_transposed(left, right):
    return lax.dot_general(
        left, right, (((1,), (1,)), ((), ())), preferred_element_type=jnp.float32
    )


def transposed_times(left, right):
    return lax.dot_general(
        left, right, (((0,), (0,)), ((), ())), preferred_element_type=jnp.float32
    )


def normalize_rows(flat_tokens, modulation_per_clip):
    values = flat_tokens.astype(jnp.float32)
    center = values - jnp.mean(values, -1, keepdims=True)
    inverse_value = lax.rsqrt(jnp.mean(center * center, -1, keepdims=True) + EPSILON)
    normalized_input = center * inverse_value
    hidden_state = (
        normalized_input * (1.0 + modulation_per_clip[1]) + modulation_per_clip[0]
    ).astype(jnp.bfloat16)
    return (normalized_input, inverse_value, hidden_state)


def projection_forward(hidden_state, qkv_full, down_full, up_full, adapter_inner_rank):
    head_size_value = up_full.shape[1]
    base_proj = jnp.dot(hidden_state, qkv_full, preferred_element_type=jnp.float32)
    low_rank_product = jnp.dot(hidden_state, down_full, preferred_element_type=jnp.float32).astype(
        jnp.bfloat16
    )
    delta_query = jnp.dot(
        low_rank_product[:, :adapter_inner_rank],
        up_full[:adapter_inner_rank],
        preferred_element_type=jnp.float32,
    )
    delta_value = jnp.dot(
        low_rank_product[:, adapter_inner_rank:],
        up_full[adapter_inner_rank:],
        preferred_element_type=jnp.float32,
    )
    query_unnormalized = base_proj[:, :head_size_value] + delta_query
    key_unnormalized = base_proj[:, head_size_value : 2 * head_size_value]
    value_row_matrix = (base_proj[:, 2 * head_size_value :] + delta_value).astype(jnp.bfloat16)
    return (low_rank_product, query_unnormalized, key_unnormalized, value_row_matrix)


def head_stats(raw_rows, head_dim):
    grouped = raw_rows.reshape(raw_rows.shape[0], -1, head_dim)
    inverse_value = lax.rsqrt(jnp.mean(grouped * grouped, -1, keepdims=True) + EPSILON)
    return (grouped, inverse_value)


def head_normed(raw_rows, head_dim):
    grouped, inverse_value = head_stats(raw_rows, head_dim)
    return (grouped * inverse_value).reshape(raw_rows.shape).astype(jnp.bfloat16)


def head_norm_back(raw_rows, incoming_grad, head_dim):
    grouped, inverse_value = head_stats(raw_rows, head_dim)
    incoming = incoming_grad.astype(jnp.float32).reshape(grouped.shape)
    inner_mean = jnp.mean(grouped * incoming, -1, keepdims=True)
    return (inverse_value * incoming - grouped * inverse_value**3 * inner_mean).reshape(
        raw_rows.shape
    )


def split_heads(rows_in, head_dim):
    frame_count, place_count, head_size_value = rows_in.shape
    return rows_in.reshape(frame_count, place_count, head_size_value // head_dim, head_dim)


def attend(query_rows, key_rows, value_row_matrix, head_dim):
    score_scale = head_dim ** (-0.5)
    query_heads = split_heads(query_rows, head_dim)
    key_heads = split_heads(key_rows, head_dim)
    value_heads = split_heads(value_row_matrix, head_dim)
    scores = (
        jnp.einsum("fphd,gphd->phfg", query_heads, key_heads, preferred_element_type=jnp.float32)
        * score_scale
    )
    expo = jnp.exp(scores)
    attention_weights = expo / jnp.sum(expo, -1, keepdims=True)
    weights_low = attention_weights.astype(jnp.bfloat16)
    attended = jnp.einsum(
        "phfg,gphd->fphd", weights_low, value_heads, preferred_element_type=jnp.float32
    ).astype(jnp.bfloat16)
    return (attended.reshape(query_rows.shape), attention_weights)


def attend_back(attended_grad, attention_weights, query_rows, key_rows, value_row_matrix, head_dim):
    score_scale = head_dim ** (-0.5)
    grad_heads = split_heads(attended_grad, head_dim)
    query_heads = split_heads(query_rows, head_dim)
    key_heads = split_heads(key_rows, head_dim)
    value_heads = split_heads(value_row_matrix, head_dim)
    weights_low = attention_weights.astype(jnp.bfloat16)
    prob_grad = jnp.einsum(
        "fphd,gphd->phfg", grad_heads, value_heads, preferred_element_type=jnp.float32
    )
    value_gradient = jnp.einsum(
        "phfg,fphd->gphd", weights_low, grad_heads, preferred_element_type=jnp.float32
    ).astype(jnp.bfloat16)
    score_grad = attention_weights * (
        prob_grad - jnp.sum(attention_weights * prob_grad, -1, keepdims=True)
    )
    score_low = (score_grad * score_scale).astype(jnp.bfloat16)
    query_grad = jnp.einsum(
        "phfg,gphd->fphd", score_low, key_heads, preferred_element_type=jnp.float32
    ).astype(jnp.bfloat16)
    key_grad = jnp.einsum(
        "phfg,fphd->gphd", score_low, query_heads, preferred_element_type=jnp.float32
    ).astype(jnp.bfloat16)
    shape_rows = query_rows.shape
    return (
        query_grad.reshape(shape_rows),
        key_grad.reshape(shape_rows),
        value_gradient.reshape(shape_rows),
    )


def projection_backward(
    query_normalized_gradient,
    key_normalized_gradient,
    value_gradient,
    query_unnormalized,
    key_unnormalized,
    hidden_state,
    low_rank_product,
    normalized_input,
    inverse_value,
    modulation_per_clip,
    qkv_full,
    down_full,
    up_full,
    adapter_inner_rank,
    head_dim,
):
    head_size_value = up_full.shape[1]
    query_back = head_norm_back(query_unnormalized, query_normalized_gradient, head_dim)
    key_back = head_norm_back(key_unnormalized, key_normalized_gradient, head_dim)
    joined_grad = jnp.concatenate(
        [query_back, key_back, value_gradient.astype(jnp.float32)], 1
    ).astype(jnp.bfloat16)
    query_block = joined_grad[:, :head_size_value]
    value_block = joined_grad[:, 2 * head_size_value :]
    up_grad = jnp.concatenate(
        [
            transposed_times(low_rank_product[:, :adapter_inner_rank], query_block),
            transposed_times(low_rank_product[:, adapter_inner_rank:], value_block),
        ],
        0,
    )
    low_grad = jnp.concatenate(
        [
            times_transposed(query_block, up_full[:adapter_inner_rank]),
            times_transposed(value_block, up_full[adapter_inner_rank:]),
        ],
        1,
    ).astype(jnp.bfloat16)
    hidden_grad = times_transposed(joined_grad, qkv_full) + times_transposed(low_grad, down_full)
    down_grad = transposed_times(hidden_state, low_grad)
    shift_gradient = jnp.sum(hidden_grad, 0)
    scale_gradient = jnp.sum(hidden_grad * normalized_input, 0)
    normed_grad = hidden_grad * (1.0 + modulation_per_clip[1])
    first_mean = jnp.mean(normed_grad, -1, keepdims=True)
    second_mean = jnp.mean(normed_grad * normalized_input, -1, keepdims=True)
    token_gradient_rows = inverse_value * (
        normed_grad - first_mean - normalized_input * second_mean
    )
    return (token_gradient_rows, shift_gradient, scale_gradient, down_grad, up_grad)


def per_device(
    tokens,
    modulation,
    query_key_value_weight,
    output_projection_weight,
    adapter_down_maps,
    adapter_up_maps,
    output_gradient,
):
    adapter_inner_rank = adapter_down_maps.shape[1] // 2
    head_dim = HEAD_SIZE
    qkv_full, out_full, down_full, up_full = (
        lax.all_gather(query_key_value_weight, "dp", axis=0, tiled=True),
        lax.all_gather(output_projection_weight, "dp", axis=1, tiled=True),
        lax.all_gather(adapter_down_maps, "dp", axis=0, tiled=True),
        lax.all_gather(adapter_up_maps, "dp", axis=0, tiled=True),
    )
    head_size_value = up_full.shape[1]
    local_shape = tokens.shape
    frame_shape = (1, local_shape[1], local_shape[2], head_size_value)
    modulation_per_clip = modulation[0]
    flat_tokens = tokens.reshape(-1, local_shape[3])
    normalized_input, inverse_value, hidden_state = normalize_rows(flat_tokens, modulation_per_clip)
    low_rank_product, query_unnormalized, key_unnormalized, value_row_matrix = projection_forward(
        hidden_state, qkv_full, down_full, up_full, adapter_inner_rank
    )
    query_rows = head_normed(query_unnormalized, head_dim)
    key_rows = head_normed(key_unnormalized, head_dim)
    upstream = output_gradient.reshape(-1, local_shape[3]).astype(jnp.float32)
    branch_grad = (upstream * modulation_per_clip[2]).astype(jnp.bfloat16)
    attended_grad = (
        times_transposed(branch_grad, out_full).astype(jnp.bfloat16).reshape(frame_shape)
    )
    query_place, key_place, value_place = (
        lax.all_to_all(
            query_rows.reshape(frame_shape), "ctx", split_axis=2, concat_axis=1, tiled=True
        ),
        lax.all_to_all(
            key_rows.reshape(frame_shape), "ctx", split_axis=2, concat_axis=1, tiled=True
        ),
        lax.all_to_all(
            value_row_matrix.reshape(frame_shape), "ctx", split_axis=2, concat_axis=1, tiled=True
        ),
    )
    attended, attention_weights = attend(query_place[0], key_place[0], value_place[0], head_dim)
    attended_frames = lax.all_to_all(attended[None], "ctx", split_axis=1, concat_axis=2, tiled=True)
    grad_place = lax.all_to_all(attended_grad, "ctx", split_axis=2, concat_axis=1, tiled=True)
    query_normalized_gradient, key_normalized_gradient, value_gradient = attend_back(
        grad_place[0], attention_weights, query_place[0], key_place[0], value_place[0], head_dim
    )
    query_back_frames, key_back_frames, value_back_frames = (
        lax.all_to_all(
            query_normalized_gradient[None], "ctx", split_axis=1, concat_axis=2, tiled=True
        ),
        lax.all_to_all(
            key_normalized_gradient[None], "ctx", split_axis=1, concat_axis=2, tiled=True
        ),
        lax.all_to_all(value_gradient[None], "ctx", split_axis=1, concat_axis=2, tiled=True),
    )
    branch_out = jnp.dot(
        attended_frames.reshape(-1, head_size_value), out_full, preferred_element_type=jnp.float32
    )
    mixed_out = (flat_tokens.astype(jnp.float32) + modulation_per_clip[2] * branch_out).astype(
        jnp.bfloat16
    )
    gate_grad = jnp.sum(upstream * branch_out, 0)
    token_gradient_rows, shift_gradient, scale_gradient, down_section, up_section = (
        projection_backward(
            query_back_frames.reshape(-1, head_size_value),
            key_back_frames.reshape(-1, head_size_value),
            value_back_frames.reshape(-1, head_size_value),
            query_unnormalized,
            key_unnormalized,
            hidden_state,
            low_rank_product,
            normalized_input,
            inverse_value,
            modulation_per_clip,
            qkv_full,
            down_full,
            up_full,
            adapter_inner_rank,
            head_dim,
        )
    )
    tokens_grad = (upstream + token_gradient_rows).astype(jnp.bfloat16)
    token_total = lax.axis_size("dp") * lax.axis_size("ctx") * flat_tokens.shape[0]
    grad_scale = token_total ** (-0.5)
    modulation_part = jnp.stack([shift_gradient, scale_gradient, gate_grad], 0)[None] * grad_scale
    down_section = down_section * grad_scale
    up_section = up_section * grad_scale
    down_total, up_total, modulation_grad = (
        lax.psum(down_section.astype(jnp.bfloat16), "ctx").astype(jnp.float32),
        lax.psum(up_section.astype(jnp.bfloat16), "ctx").astype(jnp.float32),
        lax.psum(modulation_part.astype(jnp.bfloat16), "ctx").astype(jnp.float32),
    )
    down_grad, up_grad = (
        lax.psum_scatter(
            down_total.astype(jnp.bfloat16), "dp", scatter_dimension=0, tiled=True
        ).astype(jnp.float32),
        lax.psum_scatter(
            up_total.astype(jnp.bfloat16), "dp", scatter_dimension=0, tiled=True
        ).astype(jnp.float32),
    )
    return (
        mixed_out.reshape(local_shape),
        tokens_grad.reshape(local_shape),
        modulation_grad,
        down_grad,
        up_grad,
    )


BF16 = jnp.bfloat16
F32 = jnp.float32


def dot_nn(a, b):
    return lax.dot_general(a, b, (((1,), (0,)), ((), ())), preferred_element_type=F32)


SHARED_ROWS = 16


def place(y, x, c):
    return y * 4 + x * 2 + c


def layer_kernel(
    dims,
    tokens_in, modulation_in, outgrad_in, qkv_in, out_in, down_in, up_in,
    mixed_out, tokens_grad, mod_out, down_out, up_out,
    tokens, modulation, outgrad, W, O, DT, U, H, N, BG, RAW, DS, DR, QS, QR, OS, OR, GS, GR,
    WT, LOW, LT, JG, LG, LGT, HG, AW, OF, RS, RR, US, UR, ZD, ZU, ZM, ZL,
    load_sem, local_sem, gs_sem, gr_sem, ds_sem, dr_sem, qs_sem, qr_sem, os_sem, or_sem,
    bs_sem, br_sem, rs_sem, rr_sem, us_sem, ur_sem, zs_sem, zr_sem,
):
    ndp, nctx, rows, places, width, block, heads_width, rank2, total_tokens = dims
    nh = heads_width // HEAD_SIZE
    part = rows // nctx
    head_width = 3 * HEAD_SIZE
    me = lax.axis_index("dp")
    mz = lax.axis_index("ctx")
    y, x, c = me // 4, (me // 2) % 2, me % 2
    y1, x1, c1 = 1 - y, 1 - x, 1 - c
    xn, yn, pt = place(y, x1, c), place(y1, x, c), place(y, x, c1)
    rel_owner = place((y + c) % 2, (x + 1 - c) % 2, c)
    rel_target = place((y + 1 - c) % 2, (x + c) % 2, c)
    oth_owner = rel_target
    diag = place(y1, x1, c)
    rel_r = 2 + 2 * c
    oth_r = 4 - 2 * c

    barrier = pltpu.get_barrier_semaphore()
    for t in range(1, ndp):
        pl.semaphore_signal(barrier, inc=1, device_id={"dp": lax.rem(me + t, ndp)}, device_id_type=pl.DeviceIdType.MESH)
    for t in range(1, nctx):
        pl.semaphore_signal(barrier, inc=1, device_id={"ctx": lax.rem(mz + t, nctx)}, device_id_type=pl.DeviceIdType.MESH)

    parity = mz % 2
    pair_z = mz + 1 - 2 * parity
    big = block // 48 * SHARED_ROWS
    rest = block - 2 * big
    NEAR, REST, FAR = (tuple(range(i, 3 * nh, 3)) for i in range(3))
    DOWN, UP = 3 * nh, 3 * nh + 1
    OUT = tuple(range(3 * nh + 2, 4 * nh + 2))
    items = 4 * nh + 2

    def place_of(h):
        return h // 2, h % 2 * head_width

    def piece(owner, k):
        if k in OUT:
            return O.at[owner, pl.ds((k - OUT[0]) * HEAD_SIZE, HEAD_SIZE), :]
        if k == DOWN:
            return DT.at[owner]
        if k == UP:
            return U.at[owner]
        if k in REST:
            span = pl.ds(0, rest)
        else:
            side = parity if k in NEAR else 1 - parity
            span = pl.ds(pl.multiple_of(rest + side * big, 16), big)
        pair, lo = place_of(k // 3)
        return W.at[owner, pair, span, pl.ds(lo, head_width)]

    def push(owner, k, target, s, r):
        return pltpu.make_async_remote_copy(
            src_ref=piece(owner, k), dst_ref=piece(owner, k), send_sem=gs_sem.at[s, k],
            recv_sem=gr_sem.at[r, k],
            device_id={"dp": target}, device_id_type=pl.DeviceIdType.MESH)

    def across(owner, k, s, r):
        pltpu.make_async_remote_copy(
            src_ref=piece(owner, k), dst_ref=piece(owner, k), send_sem=gs_sem.at[s, k],
            recv_sem=gr_sem.at[r, k + 2],
            device_id={"ctx": pair_z}, device_id_type=pl.DeviceIdType.MESH).start()

    def arrived(owner, k, r):
        push(owner, k, pt, 0, r).wait_recv()

    def forward(owner, k, s, r):
        push(owner, k, pt, s, r).start()

    def own_out(k):
        push(me, k, xn, 0, 2).start()
        push(me, k, yn, 1, 4).start()

    def from_sides(k):
        arrived(rel_owner, k, rel_r)
        push(rel_owner, k, rel_target, 3, 6).start()
        if k in NEAR:
            across(rel_owner, k, 7, rel_r)
        forward(rel_owner, k, 4, 1 + rel_r)
        arrived(oth_owner, k, oth_r)
        if k in NEAR:
            across(oth_owner, k, 8, oth_r)
        forward(oth_owner, k, 5, 1 + oth_r)

    def from_diag(k):
        arrived(diag, k, 6)
        if k in NEAR:
            across(diag, k, 9, 6)
        forward(diag, k, 6, 7)

    def from_far(k):
        arrived(rel_owner, k, rel_r)
        forward(rel_owner, k, 4, 1 + rel_r)
        arrived(oth_owner, k, oth_r)
        forward(oth_owner, k, 5, 1 + oth_r)

    locals_ = []
    for h in range(nh):
        pair, lo = place_of(h)
        for section in range(3):
            locals_.append(pltpu.make_async_copy(
                qkv_in.at[:, pl.ds(section * heads_width + h * HEAD_SIZE, HEAD_SIZE)],
                W.at[me, pair, :, pl.ds(lo + section * HEAD_SIZE, HEAD_SIZE)],
                local_sem.at[3 * h + section]))
    for t, (src, dst) in enumerate(((down_in, DT), (up_in, U), (out_in, O))):
        locals_.append(pltpu.make_async_copy(src, dst.at[me], local_sem.at[3 * nh + t]))
    for copy in locals_:
        copy.start()
    loads = []
    for t, (src, dst) in enumerate(((tokens_in, tokens), (outgrad_in, outgrad), (modulation_in, modulation))):
        load = pltpu.make_async_copy(src, dst, load_sem.at[t])
        load.start()
        loads.append(load)
    for copy in locals_[:3]:
        copy.wait()
    pl.semaphore_wait(barrier, ndp - 1 + nctx - 1)
    for copy in locals_[3:]:
        copy.wait()
    own_out(NEAR[0])
    own_out(NEAR[2])
    for k in (0, 1, 2, DOWN, UP) + tuple(range(3, 3 * nh)) + OUT:
        push(me, k, pt, 2, 1).start()
    for load in loads:
        load.wait()

    def cols(j):
        return pl.ds(pl.multiple_of(j * block, 128), block)

    def sum_body(j, s):
        return s + jnp.sum(tokens[:, cols(j)].astype(F32), -1, keepdims=True)

    mean = lax.fori_loop(0, ndp, sum_body, jnp.zeros((rows, 1), F32)) / width

    def var_body(j, s):
        d = tokens[:, cols(j)].astype(F32) - mean
        return s + jnp.sum(d * d, -1, keepdims=True)

    var = lax.fori_loop(0, ndp, var_body, jnp.zeros((rows, 1), F32)) / width
    rstd = lax.rsqrt(var + EPSILON)

    def norm_body(j, _):
        n = (tokens[:, cols(j)].astype(F32) - mean) * rstd
        N[j] = n
        H[j] = (n * (1.0 + modulation[1, :, cols(j)]) + modulation[0, :, cols(j)]).astype(BF16)
        BG[j] = (outgrad[:, cols(j)].astype(F32) * modulation[2, :, cols(j)]).astype(BF16)
        return 0

    lax.fori_loop(0, ndp, norm_body, 0)

    far_side = place(y, x1, c1), place(y1, x, c1), place(y1, x1, c1)
    pt_owners = ((pt, 1), (far_side[0], 3), (far_side[1], 5))
    last_owner = far_side[2]

    def grad_part(owner, h):
        WT[h] += times_transposed(BG[owner], O[owner, h * HEAD_SIZE : (h + 1) * HEAD_SIZE, :])

    def qkv_part(owner, h):
        pair, lo = place_of(h)
        RAW[h] += dot_nn(H[owner], W[owner, pair, :, lo : lo + head_width])

    def low_part(owner):
        LOW[...] += times_transposed(H[owner], DT[owner])

    def got(owner, r, kinds):
        for k in kinds:
            arrived(owner, k, r)

    frames = rows // places
    across_rows = lax.broadcasted_iota(jnp.int32, (rows, rows), 0)
    along_rows = lax.broadcasted_iota(jnp.int32, (rows, rows), 1)
    perm = jnp.where(
        along_rows == (across_rows % frames) * places + across_rows // frames, 1.0, 0.0
    ).astype(BF16)
    perm_back = jnp.where(
        across_rows == (along_rows % frames) * places + along_rows // frames, 1.0, 0.0
    ).astype(BF16)
    local_places = places // nctx
    same = jnp.where(
        (across_rows // frames) % local_places == (along_rows // frames) % local_places, 1.0, 0.0
    )

    def to_place(value):
        return dot_nn(perm, value).astype(BF16)

    def to_frame(value):
        return dot_nn(perm_back, value).astype(BF16)

    def ctx_copy(src, dst, ssem, rsem, t):
        return pltpu.make_async_remote_copy(
            src_ref=src, dst_ref=dst, send_sem=ssem, recv_sem=rsem,
            device_id={"ctx": lax.rem(mz + t, nctx)}, device_id_type=pl.DeviceIdType.MESH)

    def exchange(sent, got_ref, ssem, rsem, g):
        copies = []
        got_ref[g, mz] = sent[g, mz]
        for t in range(1, nctx):
            copy = ctx_copy(
                sent.at[g, lax.rem(mz + t, nctx)], got_ref.at[g, mz], ssem.at[g, t], rsem.at[g, t], t)
            copy.start()
            copies.append(copy)
        return copies

    def wait_all(copies):
        for copy in copies:
            copy.wait()

    def lanes(section):
        return slice(section * HEAD_SIZE, (section + 1) * HEAD_SIZE)

    def inverse_of(raw):
        return lax.rsqrt(jnp.mean(raw * raw, -1, keepdims=True) + EPSILON)

    def up_maps():
        up_rows = U[...].astype(F32).reshape(rank2, heads_width)
        in_query = lax.broadcasted_iota(jnp.int32, (rank2, heads_width), 0) < rank2 // 2
        return (
            jnp.where(in_query, up_rows, 0.0).astype(BF16),
            jnp.where(in_query, 0.0, up_rows).astype(BF16),
        )

    def send_qkv(h):
        up_query, up_value = up_maps()
        low = LOW[...].astype(BF16)
        mine = lanes(h)
        RAW[h, :, lanes(0)] += dot_nn(low, up_query[:, mine])
        RAW[h, :, lanes(2)] += dot_nn(low, up_value[:, mine])
        for section in range(3):
            raw = RAW[h, :, lanes(section)]
            if section < 2:
                raw = raw * inverse_of(raw)
            QS[h, :, :, lanes(section)] = to_place(raw.astype(BF16)).reshape(nctx, part, HEAD_SIZE)
        return exchange(QS, QR, qs_sem, qr_sem, h)

    def send_grad(h):
        DS[h] = to_place(WT[h].astype(BF16)).reshape(nctx, part, HEAD_SIZE)
        return exchange(DS, DR, ds_sem, dr_sem, h)

    scale = HEAD_SIZE ** (-0.5)

    def whole(ref, h, section=0):
        return ref[h, :, :, lanes(section)].reshape(rows, HEAD_SIZE)

    def attend(h):
        q, k, v = (whole(QR, h, section) for section in range(3))
        expo = jnp.exp(times_transposed(q, k) * scale) * same
        a = expo / jnp.sum(expo, -1, keepdims=True)
        OS[h] = dot_nn(a.astype(BF16), v).astype(BF16).reshape(nctx, part, HEAD_SIZE)
        AW[h] = a
        return exchange(OS, OR, os_sem, or_sem, h)

    def attend_back(h):
        q, k, v = (whole(QR, h, section) for section in range(3))
        d = whole(DR, h)
        a = AW[h]
        dv = transposed_times(a.astype(BF16), d)
        dp = times_transposed(d, v)
        ds = (a * (dp - jnp.sum(a * dp, -1, keepdims=True)) * scale).astype(BF16)
        dq = dot_nn(ds, k)
        dk = transposed_times(ds, q)
        for section, value in enumerate((dq, dk, dv)):
            GS[h, :, :, lanes(section)] = value.astype(BF16).reshape(nctx, part, HEAD_SIZE)
        return exchange(GS, GR, bs_sem, br_sem, h)

    def norm_back(h):
        pair, lo = place_of(h)
        for section in range(3):
            u = to_frame(whole(GR, h, section))
            if section < 2:
                raw = RAW[h, :, lanes(section)]
                inv = inverse_of(raw)
                uf = u.astype(F32)
                inner = jnp.mean(raw * uf, -1, keepdims=True)
                u = (inv * uf - raw * (inv * inv * inv) * inner).astype(BF16)
            JG[pair, :, lo + section * HEAD_SIZE : lo + (section + 1) * HEAD_SIZE] = u

    grad_scale = total_tokens ** (-0.5)

    def low_grad_part(h):
        up_query, up_value = up_maps()
        in_query = lax.broadcasted_iota(jnp.int32, (rank2, HEAD_SIZE), 0) < rank2 // 2
        mine = lanes(h)
        pair, lo = place_of(h)
        jq = JG[pair, :, lo : lo + HEAD_SIZE]
        jv = JG[pair, :, lo + 2 * HEAD_SIZE : lo + head_width]
        low = LT[...]
        up_part = jnp.where(in_query, dot_nn(low, jq), dot_nn(low, jv)) * grad_scale
        US[:, :, mine] = up_part.reshape(ndp, rank2 // ndp, HEAD_SIZE).astype(BF16)
        return times_transposed(jq, up_query[:, mine]) + times_transposed(jv, up_value[:, mine])

    RAW[...] = jnp.zeros_like(RAW)
    LOW[...] = jnp.zeros_like(LOW)
    WT[...] = jnp.zeros_like(WT)
    low_part(me)
    for h in range(nh):
        qkv_part(me, h)
        grad_part(me, h)

    def kinds(h):
        return (NEAR[h], REST[h], FAR[h])

    qkv_copies, out_copies, grad_copies, back_copies = {}, {}, {}, {}
    low_taken = set()

    def take(name, owner, h, r=None):
        if r is not None:
            got(owner, r, kinds(h))
        if name not in low_taken:
            low_taken.add(name)
            if r is not None:
                got(owner, r, (DOWN, UP))
            low_part(owner)
        qkv_part(owner, h)

    def qkv_middle(h):
        take(0, pt, h, 1)
        take(1, xn, h)
        take(2, yn, h)
        for i, (owner, r) in enumerate(pt_owners[1:]):
            take(3 + i, owner, h, r)

    def qkv_end(h):
        take(5, diag, h)
        take(6, last_owner, h, 7)
        if len(qkv_copies) == 0:
            LT[...] = LOW[...].T.astype(BF16)
        qkv_copies[h] = send_qkv(h)

    def grad_start(h):
        for owner in (xn, yn, diag):
            grad_part(owner, h)
        for owner, r in pt_owners:
            arrived(owner, OUT[h], r)
            grad_part(owner, h)

    def grad_end(h):
        arrived(last_owner, OUT[h], 7)
        grad_part(last_owner, h)
        grad_copies[h] = send_grad(h)

    def attend_step(h):
        wait_all(qkv_copies[h])
        out_copies[h] = attend(h)

    def back_step(h):
        wait_all(grad_copies[h])
        back_copies[h] = attend_back(h)

    def first_hidden(j, _):
        HG[j] = times_transposed(JG[0], W[j, 0])
        return 0

    def out_body(j, _):
        branch = dot_nn(OF[...], O[j])
        up = outgrad[:, cols(j)].astype(F32)
        mixed_out[:, cols(j)] = (
            tokens[:, cols(j)].astype(F32) + modulation[2, :, cols(j)] * branch
        ).astype(BF16)
        ZL[2, pl.ds(j, 1), :] = jnp.sum(up * branch, 0, keepdims=True) * grad_scale
        return 0

    from_sides(NEAR[0])
    own_out(NEAR[1])
    own_out(UP)
    own_out(DOWN)
    own_out(REST[1])
    from_sides(NEAR[2])
    from_diag(NEAR[0])
    own_out(REST[0])
    from_sides(NEAR[1])
    from_sides(DOWN)
    from_far(FAR[0])
    own_out(REST[2])
    from_diag(NEAR[2])
    from_sides(UP)
    from_far(FAR[2])
    from_sides(REST[0])
    from_diag(FAR[0])
    own_out(NEAR[3])
    from_diag(NEAR[1])
    from_sides(REST[2])
    from_sides(REST[1])
    from_sides(NEAR[3])
    qkv_middle(0)
    own_out(OUT[0])
    from_far(FAR[1])
    own_out(REST[3])
    from_diag(UP)
    own_out(OUT[1])
    from_diag(DOWN)
    from_diag(REST[0])
    qkv_middle(1)
    from_diag(REST[1])
    from_diag(FAR[2])
    from_diag(REST[2])
    qkv_end(0)
    from_diag(FAR[1])
    qkv_end(1)
    from_diag(NEAR[3])
    qkv_middle(2)
    from_sides(OUT[0])
    qkv_end(2)
    from_far(FAR[3])
    attend_step(0)
    from_sides(REST[3])
    from_sides(OUT[1])
    attend_step(1)
    from_diag(OUT[0])
    own_out(OUT[3])
    grad_start(0)
    from_diag(REST[3])
    from_diag(FAR[3])
    own_out(OUT[2])
    grad_end(0)
    qkv_middle(3)
    from_diag(OUT[1])
    grad_start(1)
    qkv_end(3)
    from_sides(OUT[3])
    grad_end(1)
    attend_step(2)
    from_sides(OUT[2])
    back_step(0)
    from_diag(OUT[3])
    grad_start(3)
    grad_end(3)
    attend_step(3)
    from_diag(OUT[2])
    back_step(1)
    grad_start(2)
    grad_end(2)
    back_step(3)
    for h in range(nh):
        wait_all(out_copies[h])
        OF[:, lanes(h)] = to_frame(whole(OR, h))

    lax.fori_loop(0, ndp, out_body, 0)
    back_step(2)
    for h in range(2):
        wait_all(back_copies[h])
        norm_back(h)
    lax.fori_loop(0, ndp, first_hidden, 0)
    low_grad = low_grad_part(0) + low_grad_part(1)
    z_copies = []

    def share(view, row):
        for t in range(1, nctx):
            copy = ctx_copy(view, view, zs_sem.at[row, t], zr_sem.at[row, t], t)
            copy.start()
            z_copies.append(copy)

    ZM[mz, 2] = ZL[2].astype(BF16)
    for h in range(2, nh):
        wait_all(back_copies[h])
        norm_back(h)
    share(ZM.at[mz, 2], 0)
    for h in range(2, nh):
        low_grad = low_grad + low_grad_part(h)
    LG[...] = low_grad.astype(BF16)
    LGT[...] = low_grad.T.astype(BF16)
    half = rank2 // 2

    def reduce_to(src, dst, ss, rs, to):
        copy = pltpu.make_async_remote_copy(
            src_ref=src, dst_ref=dst, send_sem=ss, recv_sem=rs,
            device_id={"dp": to}, device_id_type=pl.DeviceIdType.MESH)
        copy.start()
        return copy

    def others():
        return [(t, lax.rem(me + t, ndp)) for t in range(1, ndp)]

    up_copies = [
        reduce_to(US.at[to], UR.at[t], us_sem.at[t], ur_sem.at[t], to) for t, to in others()
    ]

    def down_part(j):
        both = (dot_nn(LGT[...], H[j]) * grad_scale).astype(BF16)
        RS[j, 0] = both[:half]
        RS[j, 1] = both[half:]

    def reduce_down(i, t, to):
        return reduce_to(RS.at[to, i], RR.at[t, i], rs_sem.at[i, t], rr_sem.at[i, t], to)

    down_copies = [[], []]
    for t, to in others():
        down_part(to)
        down_copies[0].append(reduce_down(0, t, to))
    for t, to in others():
        down_copies[1].append(reduce_down(1, t, to))
    down_part(me)

    def hidden_body(j, sums):
        first, second = sums
        hg = HG[j] + times_transposed(JG[1], W[j, 1]) + dot_nn(LG[...], DT[j])
        n = N[j]
        ZL[0, pl.ds(j, 1), :] = jnp.sum(hg, 0, keepdims=True) * grad_scale
        ZL[1, pl.ds(j, 1), :] = jnp.sum(hg * n, 0, keepdims=True) * grad_scale
        ng = hg * (1.0 + modulation[1, :, cols(j)])
        HG[j] = ng
        return (
            first + jnp.sum(ng, -1, keepdims=True),
            second + jnp.sum(ng * n, -1, keepdims=True),
        )

    def share_down(i):
        wait_all(down_copies[i])
        total = RS[me, i].astype(F32)
        for t in range(1, ndp):
            total = total + RR[t, i].astype(F32)
        ZD[mz, i] = total.astype(BF16)
        share(ZD.at[mz, i], 2 + i)

    zero = jnp.zeros((rows, 1), F32)
    first, second = lax.fori_loop(0, ndp, hidden_body, (zero, zero))
    wait_all(up_copies)
    up_sum = US[me].astype(F32)
    for t in range(1, ndp):
        up_sum = up_sum + UR[t].astype(F32)
    ZU[mz] = up_sum.astype(BF16)
    share(ZU.at[mz], 1)
    share_down(0)
    ZM[mz, pl.ds(0, 2)] = ZL[0:2].astype(BF16)
    share(ZM.at[mz, pl.ds(0, 2)], 4)
    first, second = first / width, second / width

    def last_body(j, _):
        grad = outgrad[:, cols(j)].astype(F32) + rstd * (HG[j] - first - N[j] * second)
        tokens_grad[:, cols(j)] = grad.astype(BF16)
        return 0

    lax.fori_loop(0, ndp, last_body, 0)
    share_down(1)
    wait_all(z_copies)
    down_all, up_all, mod_all = ZD[0].astype(F32), ZU[0].astype(F32), ZM[0].astype(F32)
    for z in range(1, nctx):
        down_all = down_all + ZD[z].astype(F32)
        up_all = up_all + ZU[z].astype(F32)
        mod_all = mod_all + ZM[z].astype(F32)
    for i in range(2):
        down_out[i * half : (i + 1) * half, :] = down_all[i]
    up_out[...] = up_all
    for j in range(ndp):
        for i in range(3):
            mod_out[i, :, j * block : (j + 1) * block] = mod_all[i, j : j + 1, :]

    for k in range(items):
        used = range(10) if k in NEAR else (2, 4, 5, 6) if k in FAR else range(7)
        for s in used:
            push(me, k, pt, s, 1).wait_send()


def finish_kernel(*refs):
    sem = refs[10]
    copies = [pltpu.make_async_copy(refs[i], refs[5 + i], sem.at[i]) for i in range(5)]
    for copy in copies:
        copy.start()
    for copy in copies:
        copy.wait()


def per_device_kernel(mesh_shape, *args):
    ndp, nctx = mesh_shape
    tokens, modulation, qkv, out, down, up, outgrad = args
    _, frames, places, width = tokens.shape
    rows = frames * places
    block = width // ndp
    rank2 = down.shape[1]
    hw = up.shape[1]
    part = rows // nctx
    dims = (ndp, nctx, rows, places, width, block, hw, rank2, ndp * nctx * rows)
    vm = pl.BlockSpec(memory_space=pltpu.VMEM)
    hbm = pl.BlockSpec(memory_space=pltpu.HBM)
    sem = pltpu.SemaphoreType.DMA
    ur = rank2 // ndp
    nh = hw // HEAD_SIZE
    three = 3 * HEAD_SIZE
    scratch = [
        pltpu.VMEM((rows, width), BF16),
        pltpu.VMEM((3, 1, width), F32),
        pltpu.VMEM((rows, width), BF16),
        pltpu.VMEM((ndp, nh // 2, block, 2 * three), BF16),
        pltpu.VMEM((ndp, hw, block), BF16),
        pltpu.VMEM((ndp, rank2, block), BF16),
        pltpu.VMEM((ndp, ur, hw), BF16),
        pltpu.VMEM((ndp, rows, block), BF16),
        pltpu.VMEM((ndp, rows, block), F32),
        pltpu.VMEM((ndp, rows, block), BF16),
        pltpu.VMEM((nh, rows, three), F32),
    ]
    for w in (HEAD_SIZE, three, HEAD_SIZE, three):
        scratch += [pltpu.VMEM((nh, nctx, part, w), BF16)] * 2
    scratch += [
        pltpu.VMEM((nh, rows, HEAD_SIZE), F32),
        pltpu.VMEM((rows, rank2), F32),
        pltpu.VMEM((rank2, rows), BF16),
        pltpu.VMEM((nh // 2, rows, 2 * three), BF16),
        pltpu.VMEM((rows, rank2), BF16),
        pltpu.VMEM((rank2, rows), BF16),
        pltpu.VMEM((ndp, rows, block), F32),
        pltpu.VMEM((nh, rows, rows), F32),
        pltpu.VMEM((rows, hw), BF16),
        pltpu.VMEM((ndp, 2, rank2 // 2, block), BF16),
        pltpu.VMEM((ndp, 2, rank2 // 2, block), BF16),
        pltpu.VMEM((ndp, ur, hw), BF16),
        pltpu.VMEM((ndp, ur, hw), BF16),
        pltpu.VMEM((nctx, 2, rank2 // 2, block), BF16),
        pltpu.VMEM((nctx, ur, hw), BF16),
        pltpu.VMEM((nctx, 3, ndp, block), BF16),
        pltpu.VMEM((3, ndp, block), F32),
        sem((3,)),
        sem((3 * nh + 3,)),
        sem((10, 4 * nh + 2)),
        sem((8, 4 * nh + 2)),
    ]
    scratch += [sem((nh, nctx))] * 8 + [sem((2, ndp))] * 2 + [sem((ndp,))] * 2 + [sem((5, nctx))] * 2
    results = pl.pallas_call(
        functools.partial(layer_kernel, dims),
        out_shape=(
            pltpu.VMEM((rows, width), BF16),
            pltpu.VMEM((rows, width), BF16),
            pltpu.VMEM((3, 1, width), F32),
            pltpu.VMEM((rank2, block), F32),
            pltpu.VMEM((ur, hw), F32),
        ),
        in_specs=[hbm] * 7,
        out_specs=[vm] * 5,
        scratch_shapes=scratch,
        compiler_params=pltpu.CompilerParams(
            collective_id=0, has_side_effects=True, vmem_limit_bytes=52 * 1024 * 1024
        ),
    )(
        tokens.reshape(rows, width),
        pltpu.with_memory_space_constraint(modulation.reshape(3, 1, width), pltpu.HBM),
        outgrad.reshape(rows, width),
        qkv,
        out,
        pltpu.with_memory_space_constraint(down.T, pltpu.HBM),
        pltpu.with_memory_space_constraint(up, pltpu.HBM),
    )
    mixed, tgrad, mod, dgrad, ugrad = pl.pallas_call(
        finish_kernel,
        out_shape=(
            jax.ShapeDtypeStruct((rows, width), BF16),
            jax.ShapeDtypeStruct((rows, width), BF16),
            jax.ShapeDtypeStruct((3, 1, width), F32),
            jax.ShapeDtypeStruct((rank2, block), F32),
            jax.ShapeDtypeStruct((ur, hw), F32),
        ),
        in_specs=[vm] * 5,
        out_specs=[hbm] * 5,
        scratch_shapes=[sem((5,))],
        compiler_params=pltpu.CompilerParams(vmem_limit_bytes=4 * 1024 * 1024),
    )(*results)
    return (
        mixed.reshape(tokens.shape),
        tgrad.reshape(tokens.shape),
        mod.reshape(1, 3, width),
        dgrad.T,
        ugrad,
    )


def solution(mesh):
    ndp, nctx = mesh.shape["dp"], mesh.shape["ctx"]
    body = functools.partial(per_device_kernel, (ndp, nctx)) if ndp == 8 and nctx % 2 == 0 else per_device
    return jax.shard_map(
        body,
        mesh=mesh,
        in_specs=(
            P("dp", "ctx", None, None),
            P("dp", None, None),
            P("dp", None),
            P(None, "dp"),
            P("dp", None),
            P("dp", None),
            P("dp", "ctx", None, None),
        ),
        out_specs=(
            P("dp", "ctx", None, None),
            P("dp", "ctx", None, None),
            P("dp", None, None),
            P("dp", None),
            P("dp", None),
        ),
        check_vma=False,
    )
```

```python
import functools

import jax
import jax.numpy as jnp
from jax import lax
from jax.experimental import pallas as pl
from jax.experimental.pallas import tpu as pltpu
from jax.sharding import PartitionSpec as P

HEAD_SIZE = 128


EPSILON = 1e-06


def times_transposed(left, right):
    return lax.dot_general(
        left, right, (((1,), (1,)), ((), ())), preferred_element_type=jnp.float32
    )


def transposed_times(left, right):
    return lax.dot_general(
        left, right, (((0,), (0,)), ((), ())), preferred_element_type=jnp.float32
    )


def normalize_rows(flat_tokens, modulation_per_clip):
    values = flat_tokens.astype(jnp.float32)
    center = values - jnp.mean(values, -1, keepdims=True)
    inverse_value = lax.rsqrt(jnp.mean(center * center, -1, keepdims=True) + EPSILON)
    normalized_input = center * inverse_value
    hidden_state = (
        normalized_input * (1.0 + modulation_per_clip[1]) + modulation_per_clip[0]
    ).astype(jnp.bfloat16)
    return (normalized_input, inverse_value, hidden_state)


def projection_forward(hidden_state, qkv_full, down_full, up_full, adapter_inner_rank):
    head_size_value = up_full.shape[1]
    base_proj = jnp.dot(hidden_state, qkv_full, preferred_element_type=jnp.float32)
    low_rank_product = jnp.dot(hidden_state, down_full, preferred_element_type=jnp.float32).astype(
        jnp.bfloat16
    )
    delta_query = jnp.dot(
        low_rank_product[:, :adapter_inner_rank],
        up_full[:adapter_inner_rank],
        preferred_element_type=jnp.float32,
    )
    delta_value = jnp.dot(
        low_rank_product[:, adapter_inner_rank:],
        up_full[adapter_inner_rank:],
        preferred_element_type=jnp.float32,
    )
    query_unnormalized = base_proj[:, :head_size_value] + delta_query
    key_unnormalized = base_proj[:, head_size_value : 2 * head_size_value]
    value_row_matrix = (base_proj[:, 2 * head_size_value :] + delta_value).astype(jnp.bfloat16)
    return (low_rank_product, query_unnormalized, key_unnormalized, value_row_matrix)


def head_stats(raw_rows, head_dim):
    grouped = raw_rows.reshape(raw_rows.shape[0], -1, head_dim)
    inverse_value = lax.rsqrt(jnp.mean(grouped * grouped, -1, keepdims=True) + EPSILON)
    return (grouped, inverse_value)


def head_normed(raw_rows, head_dim):
    grouped, inverse_value = head_stats(raw_rows, head_dim)
    return (grouped * inverse_value).reshape(raw_rows.shape).astype(jnp.bfloat16)


def head_norm_back(raw_rows, incoming_grad, head_dim):
    grouped, inverse_value = head_stats(raw_rows, head_dim)
    incoming = incoming_grad.astype(jnp.float32).reshape(grouped.shape)
    inner_mean = jnp.mean(grouped * incoming, -1, keepdims=True)
    return (inverse_value * incoming - grouped * inverse_value**3 * inner_mean).reshape(
        raw_rows.shape
    )


def split_heads(rows_in, head_dim):
    frame_count, place_count, head_size_value = rows_in.shape
    return rows_in.reshape(frame_count, place_count, head_size_value // head_dim, head_dim)


def attend(query_rows, key_rows, value_row_matrix, head_dim):
    score_scale = head_dim ** (-0.5)
    query_heads = split_heads(query_rows, head_dim)
    key_heads = split_heads(key_rows, head_dim)
    value_heads = split_heads(value_row_matrix, head_dim)
    scores = (
        jnp.einsum("fphd,gphd->phfg", query_heads, key_heads, preferred_element_type=jnp.float32)
        * score_scale
    )
    expo = jnp.exp(scores)
    attention_weights = expo / jnp.sum(expo, -1, keepdims=True)
    weights_low = attention_weights.astype(jnp.bfloat16)
    attended = jnp.einsum(
        "phfg,gphd->fphd", weights_low, value_heads, preferred_element_type=jnp.float32
    ).astype(jnp.bfloat16)
    return (attended.reshape(query_rows.shape), attention_weights)


def attend_back(attended_grad, attention_weights, query_rows, key_rows, value_row_matrix, head_dim):
    score_scale = head_dim ** (-0.5)
    grad_heads = split_heads(attended_grad, head_dim)
    query_heads = split_heads(query_rows, head_dim)
    key_heads = split_heads(key_rows, head_dim)
    value_heads = split_heads(value_row_matrix, head_dim)
    weights_low = attention_weights.astype(jnp.bfloat16)
    prob_grad = jnp.einsum(
        "fphd,gphd->phfg", grad_heads, value_heads, preferred_element_type=jnp.float32
    )
    value_gradient = jnp.einsum(
        "phfg,fphd->gphd", weights_low, grad_heads, preferred_element_type=jnp.float32
    ).astype(jnp.bfloat16)
    score_grad = attention_weights * (
        prob_grad - jnp.sum(attention_weights * prob_grad, -1, keepdims=True)
    )
    score_low = (score_grad * score_scale).astype(jnp.bfloat16)
    query_grad = jnp.einsum(
        "phfg,gphd->fphd", score_low, key_heads, preferred_element_type=jnp.float32
    ).astype(jnp.bfloat16)
    key_grad = jnp.einsum(
        "phfg,fphd->gphd", score_low, query_heads, preferred_element_type=jnp.float32
    ).astype(jnp.bfloat16)
    shape_rows = query_rows.shape
    return (
        query_grad.reshape(shape_rows),
        key_grad.reshape(shape_rows),
        value_gradient.reshape(shape_rows),
    )


def projection_backward(
    query_normalized_gradient,
    key_normalized_gradient,
    value_gradient,
    query_unnormalized,
    key_unnormalized,
    hidden_state,
    low_rank_product,
    normalized_input,
    inverse_value,
    modulation_per_clip,
    qkv_full,
    down_full,
    up_full,
    adapter_inner_rank,
    head_dim,
):
    head_size_value = up_full.shape[1]
    query_back = head_norm_back(query_unnormalized, query_normalized_gradient, head_dim)
    key_back = head_norm_back(key_unnormalized, key_normalized_gradient, head_dim)
    joined_grad = jnp.concatenate(
        [query_back, key_back, value_gradient.astype(jnp.float32)], 1
    ).astype(jnp.bfloat16)
    query_block = joined_grad[:, :head_size_value]
    value_block = joined_grad[:, 2 * head_size_value :]
    up_grad = jnp.concatenate(
        [
            transposed_times(low_rank_product[:, :adapter_inner_rank], query_block),
            transposed_times(low_rank_product[:, adapter_inner_rank:], value_block),
        ],
        0,
    )
    low_grad = jnp.concatenate(
        [
            times_transposed(query_block, up_full[:adapter_inner_rank]),
            times_transposed(value_block, up_full[adapter_inner_rank:]),
        ],
        1,
    ).astype(jnp.bfloat16)
    hidden_grad = times_transposed(joined_grad, qkv_full) + times_transposed(low_grad, down_full)
    down_grad = transposed_times(hidden_state, low_grad)
    shift_gradient = jnp.sum(hidden_grad, 0)
    scale_gradient = jnp.sum(hidden_grad * normalized_input, 0)
    normed_grad = hidden_grad * (1.0 + modulation_per_clip[1])
    first_mean = jnp.mean(normed_grad, -1, keepdims=True)
    second_mean = jnp.mean(normed_grad * normalized_input, -1, keepdims=True)
    token_gradient_rows = inverse_value * (
        normed_grad - first_mean - normalized_input * second_mean
    )
    return (token_gradient_rows, shift_gradient, scale_gradient, down_grad, up_grad)


def per_device(
    tokens,
    modulation,
    query_key_value_weight,
    output_projection_weight,
    adapter_down_maps,
    adapter_up_maps,
    output_gradient,
):
    adapter_inner_rank = adapter_down_maps.shape[1] // 2
    head_dim = HEAD_SIZE
    qkv_full, out_full, down_full, up_full = (
        lax.all_gather(query_key_value_weight, "dp", axis=0, tiled=True),
        lax.all_gather(output_projection_weight, "dp", axis=1, tiled=True),
        lax.all_gather(adapter_down_maps, "dp", axis=0, tiled=True),
        lax.all_gather(adapter_up_maps, "dp", axis=0, tiled=True),
    )
    head_size_value = up_full.shape[1]
    local_shape = tokens.shape
    frame_shape = (1, local_shape[1], local_shape[2], head_size_value)
    modulation_per_clip = modulation[0]
    flat_tokens = tokens.reshape(-1, local_shape[3])
    normalized_input, inverse_value, hidden_state = normalize_rows(flat_tokens, modulation_per_clip)
    low_rank_product, query_unnormalized, key_unnormalized, value_row_matrix = projection_forward(
        hidden_state, qkv_full, down_full, up_full, adapter_inner_rank
    )
    query_rows = head_normed(query_unnormalized, head_dim)
    key_rows = head_normed(key_unnormalized, head_dim)
    upstream = output_gradient.reshape(-1, local_shape[3]).astype(jnp.float32)
    branch_grad = (upstream * modulation_per_clip[2]).astype(jnp.bfloat16)
    attended_grad = (
        times_transposed(branch_grad, out_full).astype(jnp.bfloat16).reshape(frame_shape)
    )
    query_place, key_place, value_place = (
        lax.all_to_all(
            query_rows.reshape(frame_shape), "ctx", split_axis=2, concat_axis=1, tiled=True
        ),
        lax.all_to_all(
            key_rows.reshape(frame_shape), "ctx", split_axis=2, concat_axis=1, tiled=True
        ),
        lax.all_to_all(
            value_row_matrix.reshape(frame_shape), "ctx", split_axis=2, concat_axis=1, tiled=True
        ),
    )
    attended, attention_weights = attend(query_place[0], key_place[0], value_place[0], head_dim)
    attended_frames = lax.all_to_all(attended[None], "ctx", split_axis=1, concat_axis=2, tiled=True)
    grad_place = lax.all_to_all(attended_grad, "ctx", split_axis=2, concat_axis=1, tiled=True)
    query_normalized_gradient, key_normalized_gradient, value_gradient = attend_back(
        grad_place[0], attention_weights, query_place[0], key_place[0], value_place[0], head_dim
    )
    query_back_frames, key_back_frames, value_back_frames = (
        lax.all_to_all(
            query_normalized_gradient[None], "ctx", split_axis=1, concat_axis=2, tiled=True
        ),
        lax.all_to_all(
            key_normalized_gradient[None], "ctx", split_axis=1, concat_axis=2, tiled=True
        ),
        lax.all_to_all(value_gradient[None], "ctx", split_axis=1, concat_axis=2, tiled=True),
    )
    branch_out = jnp.dot(
        attended_frames.reshape(-1, head_size_value), out_full, preferred_element_type=jnp.float32
    )
    mixed_out = (flat_tokens.astype(jnp.float32) + modulation_per_clip[2] * branch_out).astype(
        jnp.bfloat16
    )
    gate_grad = jnp.sum(upstream * branch_out, 0)
    token_gradient_rows, shift_gradient, scale_gradient, down_section, up_section = (
        projection_backward(
            query_back_frames.reshape(-1, head_size_value),
            key_back_frames.reshape(-1, head_size_value),
            value_back_frames.reshape(-1, head_size_value),
            query_unnormalized,
            key_unnormalized,
            hidden_state,
            low_rank_product,
            normalized_input,
            inverse_value,
            modulation_per_clip,
            qkv_full,
            down_full,
            up_full,
            adapter_inner_rank,
            head_dim,
        )
    )
    tokens_grad = (upstream + token_gradient_rows).astype(jnp.bfloat16)
    token_total = lax.axis_size("dp") * lax.axis_size("ctx") * flat_tokens.shape[0]
    grad_scale = token_total ** (-0.5)
    modulation_part = jnp.stack([shift_gradient, scale_gradient, gate_grad], 0)[None] * grad_scale
    down_section = down_section * grad_scale
    up_section = up_section * grad_scale
    down_total, up_total, modulation_grad = (
        lax.psum(down_section.astype(jnp.bfloat16), "ctx").astype(jnp.float32),
        lax.psum(up_section.astype(jnp.bfloat16), "ctx").astype(jnp.float32),
        lax.psum(modulation_part.astype(jnp.bfloat16), "ctx").astype(jnp.float32),
    )
    down_grad, up_grad = (
        lax.psum_scatter(
            down_total.astype(jnp.bfloat16), "dp", scatter_dimension=0, tiled=True
        ).astype(jnp.float32),
        lax.psum_scatter(
            up_total.astype(jnp.bfloat16), "dp", scatter_dimension=0, tiled=True
        ).astype(jnp.float32),
    )
    return (
        mixed_out.reshape(local_shape),
        tokens_grad.reshape(local_shape),
        modulation_grad,
        down_grad,
        up_grad,
    )


BF16 = jnp.bfloat16
F32 = jnp.float32


def dot_nn(a, b):
    return lax.dot_general(a, b, (((1,), (0,)), ((), ())), preferred_element_type=F32)


SHARED_ROWS = 16


def place(y, x, c):
    return y * 4 + x * 2 + c


def layer_kernel(
    dims,
    tokens_in, modulation_in, outgrad_in, qkv_in, out_in, down_in, up_in,
    mixed_out, tokens_grad, mod_out, down_out, up_out,
    tokens, modulation, outgrad, W, O, DT, U, H, N, BG, RAW, DS, DR, QS, QR, OS, OR, GS, GR,
    WT, LOW, LT, JG, LG, LGT, HG, AW, OF, RS, RR, US, UR, ZD, ZU, ZM, ZL,
    load_sem, local_sem, gs_sem, gr_sem, ds_sem, dr_sem, qs_sem, qr_sem, os_sem, or_sem,
    bs_sem, br_sem, rs_sem, rr_sem, us_sem, ur_sem, zs_sem, zr_sem,
):
    ndp, nctx, rows, places, width, block, heads_width, rank2, total_tokens = dims
    nh = heads_width // HEAD_SIZE
    part = rows // nctx
    head_width = 3 * HEAD_SIZE
    me = lax.axis_index("dp")
    mz = lax.axis_index("ctx")
    y, x, c = me // 4, (me // 2) % 2, me % 2
    y1, x1, c1 = 1 - y, 1 - x, 1 - c
    xn, yn, pt = place(y, x1, c), place(y1, x, c), place(y, x, c1)
    rel_owner = place((y + c) % 2, (x + 1 - c) % 2, c)
    rel_target = place((y + 1 - c) % 2, (x + c) % 2, c)
    oth_owner = rel_target
    diag = place(y1, x1, c)
    rel_r = 2 + 2 * c
    oth_r = 4 - 2 * c

    barrier = pltpu.get_barrier_semaphore()
    for t in range(1, ndp):
        pl.semaphore_signal(barrier, inc=1, device_id={"dp": lax.rem(me + t, ndp)}, device_id_type=pl.DeviceIdType.MESH)
    for t in range(1, nctx):
        pl.semaphore_signal(barrier, inc=1, device_id={"ctx": lax.rem(mz + t, nctx)}, device_id_type=pl.DeviceIdType.MESH)

    parity = mz % 2
    pair_z = mz + 1 - 2 * parity
    big = block // 48 * SHARED_ROWS
    rest = block - 2 * big
    NEAR, REST, FAR = (tuple(range(i, 3 * nh, 3)) for i in range(3))
    DOWN, UP = 3 * nh, 3 * nh + 1
    OUT = tuple(range(3 * nh + 2, 4 * nh + 2))
    items = 4 * nh + 2

    def place_of(h):
        return h // 2, h % 2 * head_width

    def piece(owner, k):
        if k in OUT:
            return O.at[owner, pl.ds((k - OUT[0]) * HEAD_SIZE, HEAD_SIZE), :]
        if k == DOWN:
            return DT.at[owner]
        if k == UP:
            return U.at[owner]
        if k in REST:
            span = pl.ds(0, rest)
        else:
            side = parity if k in NEAR else 1 - parity
            span = pl.ds(pl.multiple_of(rest + side * big, 16), big)
        pair, lo = place_of(k // 3)
        return W.at[owner, pair, span, pl.ds(lo, head_width)]

    def push(owner, k, target, s, r):
        return pltpu.make_async_remote_copy(
            src_ref=piece(owner, k), dst_ref=piece(owner, k), send_sem=gs_sem.at[s, k],
            recv_sem=gr_sem.at[r, k],
            device_id={"dp": target}, device_id_type=pl.DeviceIdType.MESH)

    def across(owner, k, s, r):
        pltpu.make_async_remote_copy(
            src_ref=piece(owner, k), dst_ref=piece(owner, k), send_sem=gs_sem.at[s, k],
            recv_sem=gr_sem.at[r, k + 2],
            device_id={"ctx": pair_z}, device_id_type=pl.DeviceIdType.MESH).start()

    def arrived(owner, k, r):
        push(owner, k, pt, 0, r).wait_recv()

    def forward(owner, k, s, r):
        push(owner, k, pt, s, r).start()

    def own_out(k):
        push(me, k, xn, 0, 2).start()
        push(me, k, yn, 1, 4).start()

    def from_sides(k):
        arrived(rel_owner, k, rel_r)
        push(rel_owner, k, rel_target, 3, 6).start()
        if k in NEAR:
            across(rel_owner, k, 7, rel_r)
        forward(rel_owner, k, 4, 1 + rel_r)
        arrived(oth_owner, k, oth_r)
        if k in NEAR:
            across(oth_owner, k, 8, oth_r)
        forward(oth_owner, k, 5, 1 + oth_r)

    def from_diag(k):
        arrived(diag, k, 6)
        if k in NEAR:
            across(diag, k, 9, 6)
        forward(diag, k, 6, 7)

    def from_far(k):
        arrived(rel_owner, k, rel_r)
        forward(rel_owner, k, 4, 1 + rel_r)
        arrived(oth_owner, k, oth_r)
        forward(oth_owner, k, 5, 1 + oth_r)

    locals_ = []
    for h in range(nh):
        pair, lo = place_of(h)
        for section in range(3):
            locals_.append(pltpu.make_async_copy(
                qkv_in.at[:, pl.ds(section * heads_width + h * HEAD_SIZE, HEAD_SIZE)],
                W.at[me, pair, :, pl.ds(lo + section * HEAD_SIZE, HEAD_SIZE)],
                local_sem.at[3 * h + section]))
    for t, (src, dst) in enumerate(((down_in, DT), (up_in, U), (out_in, O))):
        locals_.append(pltpu.make_async_copy(src, dst.at[me], local_sem.at[3 * nh + t]))
    for copy in locals_:
        copy.start()
    loads = []
    for t, (src, dst) in enumerate(((tokens_in, tokens), (outgrad_in, outgrad), (modulation_in, modulation))):
        load = pltpu.make_async_copy(src, dst, load_sem.at[t])
        load.start()
        loads.append(load)
    for copy in locals_[:3]:
        copy.wait()
    pl.semaphore_wait(barrier, ndp - 1 + nctx - 1)
    own_out(NEAR[0])
    for copy in locals_[3:]:
        copy.wait()
    own_out(NEAR[2])
    for k in (0, 1, 2, DOWN, UP) + tuple(range(3, 3 * nh)) + OUT:
        push(me, k, pt, 2, 1).start()
    for load in loads:
        load.wait()

    def cols(j):
        return pl.ds(pl.multiple_of(j * block, 128), block)

    def sum_body(j, s):
        return s + jnp.sum(tokens[:, cols(j)].astype(F32), -1, keepdims=True)

    mean = lax.fori_loop(0, ndp, sum_body, jnp.zeros((rows, 1), F32)) / width

    def var_body(j, s):
        d = tokens[:, cols(j)].astype(F32) - mean
        return s + jnp.sum(d * d, -1, keepdims=True)

    var = lax.fori_loop(0, ndp, var_body, jnp.zeros((rows, 1), F32)) / width
    rstd = lax.rsqrt(var + EPSILON)

    def norm_body(j, _):
        n = (tokens[:, cols(j)].astype(F32) - mean) * rstd
        N[j] = n
        H[j] = (n * (1.0 + modulation[1, :, cols(j)]) + modulation[0, :, cols(j)]).astype(BF16)
        BG[j] = (outgrad[:, cols(j)].astype(F32) * modulation[2, :, cols(j)]).astype(BF16)
        return 0

    lax.fori_loop(0, ndp, norm_body, 0)

    far_side = place(y, x1, c1), place(y1, x, c1), place(y1, x1, c1)
    pt_owners = ((pt, 1), (far_side[0], 3), (far_side[1], 5))
    last_owner = far_side[2]

    def grad_part(owner, h):
        WT[h] += times_transposed(BG[owner], O[owner, h * HEAD_SIZE : (h + 1) * HEAD_SIZE, :])

    def qkv_part(owner, h):
        pair, lo = place_of(h)
        RAW[h] += dot_nn(H[owner], W[owner, pair, :, lo : lo + head_width])

    def low_part(owner):
        LOW[...] += times_transposed(H[owner], DT[owner])

    def got(owner, r, kinds):
        for k in kinds:
            arrived(owner, k, r)

    frames = rows // places
    across_rows = lax.broadcasted_iota(jnp.int32, (rows, rows), 0)
    along_rows = lax.broadcasted_iota(jnp.int32, (rows, rows), 1)
    perm = jnp.where(
        along_rows == (across_rows % frames) * places + across_rows // frames, 1.0, 0.0
    ).astype(BF16)
    perm_back = jnp.where(
        across_rows == (along_rows % frames) * places + along_rows // frames, 1.0, 0.0
    ).astype(BF16)
    local_places = places // nctx
    same = jnp.where(
        (across_rows // frames) % local_places == (along_rows // frames) % local_places, 1.0, 0.0
    )

    def to_place(value):
        return dot_nn(perm, value).astype(BF16)

    def to_frame(value):
        return dot_nn(perm_back, value).astype(BF16)

    def ctx_copy(src, dst, ssem, rsem, t):
        return pltpu.make_async_remote_copy(
            src_ref=src, dst_ref=dst, send_sem=ssem, recv_sem=rsem,
            device_id={"ctx": lax.rem(mz + t, nctx)}, device_id_type=pl.DeviceIdType.MESH)

    def exchange(sent, got_ref, ssem, rsem, g):
        copies = []
        got_ref[g, mz] = sent[g, mz]
        for t in range(1, nctx):
            copy = ctx_copy(
                sent.at[g, lax.rem(mz + t, nctx)], got_ref.at[g, mz], ssem.at[g, t], rsem.at[g, t], t)
            copy.start()
            copies.append(copy)
        return copies

    def wait_all(copies):
        for copy in copies:
            copy.wait()

    def lanes(section):
        return slice(section * HEAD_SIZE, (section + 1) * HEAD_SIZE)

    def inverse_of(raw):
        return lax.rsqrt(jnp.mean(raw * raw, -1, keepdims=True) + EPSILON)

    def up_maps():
        up_rows = U[...].astype(F32).reshape(rank2, heads_width)
        in_query = lax.broadcasted_iota(jnp.int32, (rank2, heads_width), 0) < rank2 // 2
        return (
            jnp.where(in_query, up_rows, 0.0).astype(BF16),
            jnp.where(in_query, 0.0, up_rows).astype(BF16),
        )

    def send_qkv(h):
        up_query, up_value = up_maps()
        low = LOW[...].astype(BF16)
        mine = lanes(h)
        RAW[h, :, lanes(0)] += dot_nn(low, up_query[:, mine])
        RAW[h, :, lanes(2)] += dot_nn(low, up_value[:, mine])
        for section in range(3):
            raw = RAW[h, :, lanes(section)]
            if section < 2:
                raw = raw * inverse_of(raw)
            QS[h, :, :, lanes(section)] = to_place(raw.astype(BF16)).reshape(nctx, part, HEAD_SIZE)
        return exchange(QS, QR, qs_sem, qr_sem, h)

    def send_grad(h):
        DS[h] = to_place(WT[h].astype(BF16)).reshape(nctx, part, HEAD_SIZE)
        return exchange(DS, DR, ds_sem, dr_sem, h)

    scale = HEAD_SIZE ** (-0.5)

    def whole(ref, h, section=0):
        return ref[h, :, :, lanes(section)].reshape(rows, HEAD_SIZE)

    def attend(h):
        q, k, v = (whole(QR, h, section) for section in range(3))
        expo = jnp.exp(times_transposed(q, k) * scale) * same
        a = expo / jnp.sum(expo, -1, keepdims=True)
        OS[h] = dot_nn(a.astype(BF16), v).astype(BF16).reshape(nctx, part, HEAD_SIZE)
        AW[h] = a
        return exchange(OS, OR, os_sem, or_sem, h)

    def attend_back(h):
        q, k, v = (whole(QR, h, section) for section in range(3))
        d = whole(DR, h)
        a = AW[h]
        dv = transposed_times(a.astype(BF16), d)
        dp = times_transposed(d, v)
        ds = (a * (dp - jnp.sum(a * dp, -1, keepdims=True)) * scale).astype(BF16)
        dq = dot_nn(ds, k)
        dk = transposed_times(ds, q)
        for section, value in enumerate((dq, dk, dv)):
            GS[h, :, :, lanes(section)] = value.astype(BF16).reshape(nctx, part, HEAD_SIZE)
        return exchange(GS, GR, bs_sem, br_sem, h)

    def norm_back(h):
        pair, lo = place_of(h)
        for section in range(3):
            u = to_frame(whole(GR, h, section))
            if section < 2:
                raw = RAW[h, :, lanes(section)]
                inv = inverse_of(raw)
                uf = u.astype(F32)
                inner = jnp.mean(raw * uf, -1, keepdims=True)
                u = (inv * uf - raw * (inv * inv * inv) * inner).astype(BF16)
            JG[pair, :, lo + section * HEAD_SIZE : lo + (section + 1) * HEAD_SIZE] = u

    grad_scale = total_tokens ** (-0.5)

    def low_grad_part(h):
        up_query, up_value = up_maps()
        in_query = lax.broadcasted_iota(jnp.int32, (rank2, HEAD_SIZE), 0) < rank2 // 2
        mine = lanes(h)
        pair, lo = place_of(h)
        jq = JG[pair, :, lo : lo + HEAD_SIZE]
        jv = JG[pair, :, lo + 2 * HEAD_SIZE : lo + head_width]
        low = LT[...]
        up_part = jnp.where(in_query, dot_nn(low, jq), dot_nn(low, jv)) * grad_scale
        US[:, :, mine] = up_part.reshape(ndp, rank2 // ndp, HEAD_SIZE).astype(BF16)
        return times_transposed(jq, up_query[:, mine]) + times_transposed(jv, up_value[:, mine])

    RAW[...] = jnp.zeros_like(RAW)
    LOW[...] = jnp.zeros_like(LOW)
    WT[...] = jnp.zeros_like(WT)
    low_part(me)
    for h in range(nh):
        qkv_part(me, h)
        grad_part(me, h)

    def kinds(h):
        return (NEAR[h], REST[h], FAR[h])

    qkv_copies, out_copies, grad_copies, back_copies = {}, {}, {}, {}
    low_taken = set()

    def take(name, owner, h, r=None):
        if r is not None:
            got(owner, r, kinds(h))
        if name not in low_taken:
            low_taken.add(name)
            if r is not None:
                got(owner, r, (DOWN, UP))
            low_part(owner)
        qkv_part(owner, h)

    def qkv_middle(h):
        take(0, pt, h, 1)
        take(1, xn, h)
        take(2, yn, h)
        for i, (owner, r) in enumerate(pt_owners[1:]):
            take(3 + i, owner, h, r)

    def qkv_end(h):
        take(5, diag, h)
        take(6, last_owner, h, 7)
        if len(qkv_copies) == 0:
            LT[...] = LOW[...].T.astype(BF16)
        qkv_copies[h] = send_qkv(h)

    def grad_start(h):
        for owner in (xn, yn, diag):
            grad_part(owner, h)
        for owner, r in pt_owners:
            arrived(owner, OUT[h], r)
            grad_part(owner, h)

    def grad_end(h):
        arrived(last_owner, OUT[h], 7)
        grad_part(last_owner, h)
        grad_copies[h] = send_grad(h)

    def attend_step(h):
        wait_all(qkv_copies[h])
        out_copies[h] = attend(h)

    def back_step(h):
        wait_all(grad_copies[h])
        back_copies[h] = attend_back(h)

    def first_hidden(j, _):
        HG[j] = times_transposed(JG[0], W[j, 0])
        return 0

    def out_body(j, _):
        branch = dot_nn(OF[...], O[j])
        up = outgrad[:, cols(j)].astype(F32)
        mixed_out[:, cols(j)] = (
            tokens[:, cols(j)].astype(F32) + modulation[2, :, cols(j)] * branch
        ).astype(BF16)
        ZL[2, pl.ds(j, 1), :] = jnp.sum(up * branch, 0, keepdims=True) * grad_scale
        return 0

    from_sides(NEAR[0])
    own_out(NEAR[1])
    own_out(UP)
    own_out(DOWN)
    own_out(REST[1])
    from_sides(NEAR[2])
    from_diag(NEAR[0])
    own_out(REST[0])
    from_sides(NEAR[1])
    from_sides(DOWN)
    from_far(FAR[0])
    own_out(REST[2])
    from_diag(NEAR[2])
    from_sides(UP)
    from_far(FAR[2])
    from_sides(REST[0])
    from_diag(FAR[0])
    own_out(NEAR[3])
    from_diag(NEAR[1])
    from_sides(REST[2])
    from_sides(REST[1])
    from_sides(NEAR[3])
    qkv_middle(0)
    own_out(OUT[0])
    from_far(FAR[1])
    own_out(REST[3])
    from_diag(UP)
    own_out(OUT[1])
    from_diag(DOWN)
    from_diag(REST[0])
    qkv_middle(1)
    from_diag(REST[1])
    from_diag(FAR[2])
    from_diag(REST[2])
    qkv_end(0)
    from_diag(FAR[1])
    qkv_end(1)
    from_diag(NEAR[3])
    qkv_middle(2)
    from_sides(OUT[0])
    qkv_end(2)
    from_far(FAR[3])
    attend_step(0)
    from_sides(REST[3])
    from_sides(OUT[1])
    attend_step(1)
    from_diag(OUT[0])
    own_out(OUT[3])
    grad_start(0)
    from_diag(REST[3])
    from_diag(FAR[3])
    own_out(OUT[2])
    grad_end(0)
    qkv_middle(3)
    from_diag(OUT[1])
    grad_start(1)
    qkv_end(3)
    from_sides(OUT[3])
    grad_end(1)
    attend_step(2)
    from_sides(OUT[2])
    back_step(0)
    from_diag(OUT[3])
    grad_start(3)
    grad_end(3)
    attend_step(3)
    from_diag(OUT[2])
    grad_start(2)
    grad_end(2)
    back_step(1)
    back_step(3)
    for h in range(nh):
        wait_all(out_copies[h])
        OF[:, lanes(h)] = to_frame(whole(OR, h))

    lax.fori_loop(0, ndp, out_body, 0)
    back_step(2)
    for h in range(2):
        wait_all(back_copies[h])
        norm_back(h)
    lax.fori_loop(0, ndp, first_hidden, 0)
    low_grad = low_grad_part(0) + low_grad_part(1)
    z_copies = []

    def share(view, row):
        for t in range(1, nctx):
            copy = ctx_copy(view, view, zs_sem.at[row, t], zr_sem.at[row, t], t)
            copy.start()
            z_copies.append(copy)

    for i in range(2):
        ZM[i, mz, 2] = ZL[2, i * (ndp // 2) : (i + 1) * (ndp // 2)].astype(BF16)
    for h in range(2, nh):
        wait_all(back_copies[h])
        norm_back(h)
    for i in range(2):
        share(ZM.at[i, mz, 2], i)
    for h in range(2, nh):
        low_grad = low_grad + low_grad_part(h)
    LG[...] = low_grad.astype(BF16)
    LGT[...] = low_grad.T.astype(BF16)
    half = rank2 // 2

    def reduce_to(src, dst, ss, rs, to):
        copy = pltpu.make_async_remote_copy(
            src_ref=src, dst_ref=dst, send_sem=ss, recv_sem=rs,
            device_id={"dp": to}, device_id_type=pl.DeviceIdType.MESH)
        copy.start()
        return copy

    def others():
        return [(t, lax.rem(me + t, ndp)) for t in range(1, ndp)]

    up_copies = [
        reduce_to(US.at[to], UR.at[t], us_sem.at[t], ur_sem.at[t], to) for t, to in others()
    ]

    def down_part(j):
        both = (dot_nn(LGT[...], H[j]) * grad_scale).astype(BF16)
        RS[j, 0] = both[:half]
        RS[j, 1] = both[half:]

    def reduce_down(i, t, to):
        return reduce_to(RS.at[to, i], RR.at[t, i], rs_sem.at[i, t], rr_sem.at[i, t], to)

    down_copies = [[], []]
    for t, to in others():
        down_part(to)
        down_copies[0].append(reduce_down(0, t, to))
    for t, to in others():
        down_copies[1].append(reduce_down(1, t, to))
    down_part(me)

    def hidden_body(j, sums):
        first, second = sums
        hg = HG[j] + times_transposed(JG[1], W[j, 1]) + dot_nn(LG[...], DT[j])
        n = N[j]
        ZL[0, pl.ds(j, 1), :] = jnp.sum(hg, 0, keepdims=True) * grad_scale
        ZL[1, pl.ds(j, 1), :] = jnp.sum(hg * n, 0, keepdims=True) * grad_scale
        ng = hg * (1.0 + modulation[1, :, cols(j)])
        HG[j] = ng
        return (
            first + jnp.sum(ng, -1, keepdims=True),
            second + jnp.sum(ng * n, -1, keepdims=True),
        )

    def share_down(i):
        wait_all(down_copies[i])
        total = RS[me, i].astype(F32)
        for t in range(1, ndp):
            total = total + RR[t, i].astype(F32)
        ZD[mz, i] = total.astype(BF16)
        share(ZD.at[mz, i], 3 + i)

    zero = jnp.zeros((rows, 1), F32)
    middle = ndp // 2

    def share_sums(i):
        ZM[i, mz, pl.ds(0, 2)] = ZL[0:2, i * middle : (i + 1) * middle].astype(BF16)
        share(ZM.at[i, mz, pl.ds(0, 2)], 5 + i)

    sums = lax.fori_loop(0, middle, hidden_body, (zero, zero))
    share_sums(0)
    first, second = lax.fori_loop(middle, ndp, hidden_body, sums)
    wait_all(up_copies)
    up_sum = US[me].astype(F32)
    for t in range(1, ndp):
        up_sum = up_sum + UR[t].astype(F32)
    ZU[mz] = up_sum.astype(BF16)
    share(ZU.at[mz], 2)
    share_down(0)
    share_sums(1)
    first, second = first / width, second / width

    def last_body(j, _):
        grad = outgrad[:, cols(j)].astype(F32) + rstd * (HG[j] - first - N[j] * second)
        tokens_grad[:, cols(j)] = grad.astype(BF16)
        return 0

    lax.fori_loop(0, ndp, last_body, 0)
    share_down(1)
    wait_all(z_copies)
    down_all, up_all = ZD[0].astype(F32), ZU[0].astype(F32)
    for z in range(1, nctx):
        down_all = down_all + ZD[z].astype(F32)
        up_all = up_all + ZU[z].astype(F32)
    for i in range(2):
        down_out[i * half : (i + 1) * half, :] = down_all[i]
    up_out[...] = up_all
    for j in range(ndp):
        mod_all = ZM[j // middle, 0].astype(F32)
        for z in range(1, nctx):
            mod_all = mod_all + ZM[j // middle, z].astype(F32)
        row = j % middle
        for i in range(3):
            mod_out[i, :, j * block : (j + 1) * block] = mod_all[i, row : row + 1, :]

    for k in range(items):
        used = range(10) if k in NEAR else (2, 4, 5, 6) if k in FAR else range(7)
        for s in used:
            push(me, k, pt, s, 1).wait_send()


def finish_kernel(*refs):
    sem = refs[10]
    copies = [pltpu.make_async_copy(refs[i], refs[5 + i], sem.at[i]) for i in range(5)]
    for copy in copies:
        copy.start()
    for copy in copies:
        copy.wait()


def per_device_kernel(mesh_shape, *args):
    ndp, nctx = mesh_shape
    tokens, modulation, qkv, out, down, up, outgrad = args
    _, frames, places, width = tokens.shape
    rows = frames * places
    block = width // ndp
    rank2 = down.shape[1]
    hw = up.shape[1]
    part = rows // nctx
    dims = (ndp, nctx, rows, places, width, block, hw, rank2, ndp * nctx * rows)
    vm = pl.BlockSpec(memory_space=pltpu.VMEM)
    hbm = pl.BlockSpec(memory_space=pltpu.HBM)
    sem = pltpu.SemaphoreType.DMA
    ur = rank2 // ndp
    nh = hw // HEAD_SIZE
    three = 3 * HEAD_SIZE
    scratch = [
        pltpu.VMEM((rows, width), BF16),
        pltpu.VMEM((3, 1, width), F32),
        pltpu.VMEM((rows, width), BF16),
        pltpu.VMEM((ndp, nh // 2, block, 2 * three), BF16),
        pltpu.VMEM((ndp, hw, block), BF16),
        pltpu.VMEM((ndp, rank2, block), BF16),
        pltpu.VMEM((ndp, ur, hw), BF16),
        pltpu.VMEM((ndp, rows, block), BF16),
        pltpu.VMEM((ndp, rows, block), F32),
        pltpu.VMEM((ndp, rows, block), BF16),
        pltpu.VMEM((nh, rows, three), F32),
    ]
    for w in (HEAD_SIZE, three, HEAD_SIZE, three):
        scratch += [pltpu.VMEM((nh, nctx, part, w), BF16)] * 2
    scratch += [
        pltpu.VMEM((nh, rows, HEAD_SIZE), F32),
        pltpu.VMEM((rows, rank2), F32),
        pltpu.VMEM((rank2, rows), BF16),
        pltpu.VMEM((nh // 2, rows, 2 * three), BF16),
        pltpu.VMEM((rows, rank2), BF16),
        pltpu.VMEM((rank2, rows), BF16),
        pltpu.VMEM((ndp, rows, block), F32),
        pltpu.VMEM((nh, rows, rows), F32),
        pltpu.VMEM((rows, hw), BF16),
        pltpu.VMEM((ndp, 2, rank2 // 2, block), BF16),
        pltpu.VMEM((ndp, 2, rank2 // 2, block), BF16),
        pltpu.VMEM((ndp, ur, hw), BF16),
        pltpu.VMEM((ndp, ur, hw), BF16),
        pltpu.VMEM((nctx, 2, rank2 // 2, block), BF16),
        pltpu.VMEM((nctx, ur, hw), BF16),
        pltpu.VMEM((2, nctx, 3, ndp // 2, block), BF16),
        pltpu.VMEM((3, ndp, block), F32),
        sem((3,)),
        sem((3 * nh + 3,)),
        sem((10, 4 * nh + 2)),
        sem((8, 4 * nh + 2)),
    ]
    scratch += [sem((nh, nctx))] * 8 + [sem((2, ndp))] * 2 + [sem((ndp,))] * 2 + [sem((7, nctx))] * 2
    results = pl.pallas_call(
        functools.partial(layer_kernel, dims),
        out_shape=(
            pltpu.VMEM((rows, width), BF16),
            pltpu.VMEM((rows, width), BF16),
            pltpu.VMEM((3, 1, width), F32),
            pltpu.VMEM((rank2, block), F32),
            pltpu.VMEM((ur, hw), F32),
        ),
        in_specs=[hbm] * 7,
        out_specs=[vm] * 5,
        scratch_shapes=scratch,
        compiler_params=pltpu.CompilerParams(
            collective_id=0, has_side_effects=True, vmem_limit_bytes=52 * 1024 * 1024
        ),
    )(
        tokens.reshape(rows, width),
        pltpu.with_memory_space_constraint(modulation.reshape(3, 1, width), pltpu.HBM),
        outgrad.reshape(rows, width),
        qkv,
        out,
        pltpu.with_memory_space_constraint(down.T, pltpu.HBM),
        pltpu.with_memory_space_constraint(up, pltpu.HBM),
    )
    mixed, tgrad, mod, dgrad, ugrad = pl.pallas_call(
        finish_kernel,
        out_shape=(
            jax.ShapeDtypeStruct((rows, width), BF16),
            jax.ShapeDtypeStruct((rows, width), BF16),
            jax.ShapeDtypeStruct((3, 1, width), F32),
            jax.ShapeDtypeStruct((rank2, block), F32),
            jax.ShapeDtypeStruct((ur, hw), F32),
        ),
        in_specs=[vm] * 5,
        out_specs=[hbm] * 5,
        scratch_shapes=[sem((5,))],
        compiler_params=pltpu.CompilerParams(vmem_limit_bytes=4 * 1024 * 1024),
    )(*results)
    return (
        mixed.reshape(tokens.shape),
        tgrad.reshape(tokens.shape),
        mod.reshape(1, 3, width),
        dgrad.T,
        ugrad,
    )


def solution(mesh):
    ndp, nctx = mesh.shape["dp"], mesh.shape["ctx"]
    body = functools.partial(per_device_kernel, (ndp, nctx)) if ndp == 8 and nctx % 2 == 0 else per_device
    return jax.shard_map(
        body,
        mesh=mesh,
        in_specs=(
            P("dp", "ctx", None, None),
            P("dp", None, None),
            P("dp", None),
            P(None, "dp"),
            P("dp", None),
            P("dp", None),
            P("dp", "ctx", None, None),
        ),
        out_specs=(
            P("dp", "ctx", None, None),
            P("dp", "ctx", None, None),
            P("dp", None, None),
            P("dp", None),
            P("dp", None),
        ),
        check_vma=False,
    )
```
